1024 devices in a mesh: section: 64 (over z, y_hi), fsdp: 4 (over y_lo, core), tp: 4 (over x).
Axes of the slice: x: 4, y: 4 (y_hi: 2, y_lo: 2; y = y_hi * 2 + y_lo), z: 32, core: 2. Of those that a mesh axis runs over, the one named last changes fastest.
Arguments:
- stash: bfloat16 [64, 4, 512, 2304], P('section', None, 'fsdp'), may hold values from -6 to 6
- grad_now: bfloat16 [64, 512, 2304], P('section', 'fsdp'), may hold values from -6 to 6
- grad_top: bfloat16 [2, 512, 2304], P(None, 'fsdp'), may hold values from -6 to 6
- order: int32 [64, 4], P('section'), may hold values from 0 to 3, each once within a row
- gain: float32 [64, 2304], P('section'), may hold values from 0.5 to 1.5
- weight: bfloat16 [64, 2304, 2048], P('section', 'fsdp', 'tp'), may hold values from -0.125 to 0.125
Outputs:
- grad_held: bfloat16 [64, 512, 2304], P('section', 'fsdp')
- weight_grad: float32 [64, 2304, 2048], P('section', 'fsdp', 'tp')
The draws below stay inside these ranges and needn't reach their ends.
Inputs may be any that keep to these rules, and one draw needn't show every extreme that they name: Each row of order names every kept micro-batch once.
All inputs are finite; a program needn't handle non-finite values.
Results may differ from the reference program's by a relative error of at most 0.013.
Values may be sent and summed in bfloat16 or wider, within the bound.
No kernel may reach another device: no remote copies, remote signals or barrier semaphores. Data moves between devices by JAX's collectives and lax.ppermute only.
A program may use at most 64 MiB of HBM per device.

```python
import jax
import jax.numpy as jnp
from jax import lax

D = 2304
INNER = 2048
MB = 4
TICKS = 2
SECTIONS = 64
TOKENS = 512
N_TP = 4


def level_of(key, extent, pieces, least, largest):
    def one(axis_at, blocks):
        heights = jax.random.uniform(jax.random.fold_in(jax.random.fold_in(key, 6), axis_at), (blocks,), jnp.float32, least / len(pieces), largest / len(pieces))
        return jnp.repeat(jnp.exp(heights), extent[axis_at] // blocks).reshape((-1,) + (1,) * (len(extent) - axis_at - 1))

    level = one(*pieces[0])
    for cut in pieces[1:]:
        level = level * one(*cut)
    return level


def scatter_about(key, extent, spread, limit, cuts=(), kind=jnp.bfloat16):
    loudness = level_of(key, extent, cuts, -0.22, 0.18) if cuts else 1.0
    drawn = jax.random.normal(key, extent, jnp.float32) * spread * loudness
    return jnp.minimum(jnp.maximum(drawn, -limit), limit).astype(kind)


def setup_inputs(seed: int = 0) -> dict:
    seeds = jax.random.split(jax.random.key(seed), 7)
    stash = scatter_about(seeds[0], (SECTIONS, MB, TOKENS, D), 1.0, 6.0, ((0, 64), (2, 4)))
    grad_now = scatter_about(seeds[1], (SECTIONS, TOKENS, D), 1.0, 6.0, ((0, 64), (1, 4)))
    grad_top = scatter_about(seeds[2], (TICKS, TOKENS, D), 1.0, 6.0, ((1, 4),))
    order = jax.vmap(lambda own: jax.random.permutation(own, MB))(jax.random.split(seeds[3], SECTIONS)).reshape((SECTIONS, MB)).astype(jnp.int32)
    gain = jnp.clip(1.0 + 0.1 * jax.random.normal(seeds[4], (SECTIONS, D), jnp.float32), 0.5, 1.5)
    weight = scatter_about(seeds[5], (SECTIONS, D, INNER), D ** -0.5, 0.125, ((0, 64), (1, 4), (2, 4)))
    return dict(stash=stash, grad_now=grad_now, grad_top=grad_top, order=order, gain=gain, weight=weight)


norm_eps = 1e-06

def gelu_tanh(values):
    return jax.nn.gelu(values, approximate=True)

def section_tick(section_in, grad_in, section_gain, section_weight):
    values = section_in.astype(jnp.float32)
    inv_rms = lax.rsqrt(lax.optimization_barrier(jnp.mean(values * values, axis=-1, keepdims=True)) + norm_eps)
    scaled = values * inv_rms
    normed = (scaled * section_gain).astype(jnp.bfloat16)
    hidden = jnp.dot(normed, section_weight, preferred_element_type=jnp.float32)
    backed = jnp.dot(grad_in, section_weight, preferred_element_type=jnp.float32)
    activated, pullback = jax.vjp(gelu_tanh, hidden)
    grad_pre = pullback(backed)[0].astype(jnp.bfloat16)
    activated = activated.astype(jnp.bfloat16)
    group = section_weight.shape[1] // N_TP
    total = jnp.zeros(values.shape, jnp.float32)
    for member in range(N_TP):
        left = grad_pre[:, member * group:(member + 1) * group]
        right = section_weight[:, member * group:(member + 1) * group]
        partial_dh = lax.dot_general(left, right, (((1,), (1,)), ((), ())), preferred_element_type=jnp.float32)
        rounded = lax.optimization_barrier(partial_dh.astype(jnp.bfloat16))
        total = total + rounded.astype(jnp.float32)
    gained = section_gain * total
    inner_mean = lax.optimization_barrier(jnp.mean(gained * scaled, axis=-1, keepdims=True))
    grad_out = (grad_in.astype(jnp.float32) + inv_rms * (gained - scaled * inner_mean)).astype(jnp.bfloat16)
    return (grad_out, normed, grad_pre, activated)

def reference(stash, grad_now, grad_top, order, gain, weight):
    held = grad_now
    lhs_parts = []
    rhs_parts = []
    for tick_id in range(TICKS):

        def per_section(items):
            section_stash, section_order, grad_in, section_gain, section_weight = items
            slot_id = section_order[tick_id].astype(jnp.int32)
            section_in = lax.dynamic_index_in_dim(section_stash, slot_id, 0, keepdims=False)
            return section_tick(section_in, grad_in, section_gain, section_weight)
        grad_out, normed, grad_pre, activated = lax.map(per_section, (stash, order, held, gain, weight))
        lhs_parts.append(normed)
        lhs_parts.append(held)
        rhs_parts.append(grad_pre)
        rhs_parts.append(activated)
        held = jnp.concatenate([grad_out[1:], grad_top[tick_id][None]], axis=0)
    lhs_all = jnp.concatenate(lhs_parts, axis=1)
    rhs_all = jnp.concatenate(rhs_parts, axis=1)

    def section_grad(items):
        left, right = items
        return lax.dot_general(left, right, (((0,), (0,)), ((), ())), preferred_element_type=jnp.float32)
    weight_grad = lax.map(section_grad, (lhs_all, rhs_all))
    return (held, weight_grad)
```

```python
import functools

import jax
import jax.numpy as jnp
from jax import lax
from jax.experimental import pallas as pl
from jax.experimental.pallas import tpu as pltpu
from jax.sharding import PartitionSpec as P


norm_eps = 1e-06
f32 = jnp.float32
bf16 = jnp.bfloat16
gelu_scale = 0.7978845608028654
gelu_cubic = 0.044715
vmem_budget = 16 * 1024 * 1024


def dot_nn(left, right):
    return jnp.dot(left, right, preferred_element_type=f32)


def dot_nt(left, right):
    return lax.dot_general(left, right, (((1,), (1,)), ((), ())), preferred_element_type=f32)


def dot_tn(left, right):
    return lax.dot_general(left, right, (((0,), (0,)), ((), ())), preferred_element_type=f32)


def gelu_and_slope(values):
    squared = values * values
    tanh = jnp.tanh(gelu_scale * values * (1.0 + gelu_cubic * squared))
    half = 0.5 * (1.0 + tanh)
    slope = half + 0.5 * values * (1.0 - tanh * tanh) * (
        gelu_scale * (1.0 + 3.0 * gelu_cubic * squared)
    )
    return values * half, slope


def cost(flops, outs, args):
    size = sum(v.size * v.dtype.itemsize for v in jax.tree.leaves((outs, args)))
    return pl.CostEstimate(flops=int(flops), bytes_accessed=size, transcendentals=0)


def call(kernel, flops, outs, *args):
    return pl.pallas_call(
        kernel,
        out_shape=outs,
        cost_estimate=cost(flops, outs, args),
        compiler_params=pltpu.CompilerParams(vmem_limit_bytes=vmem_budget),
    )(*args)


def cut_blocks(values, ref):
    count, width = ref.shape[0], ref.shape[2]
    for b in range(count):
        ref[b] = values[:, b * width : (b + 1) * width]


def prepare_kernel(order_ref, stash_ref, gain_ref, h_ref, x_ref, inv_ref):
    values = stash_ref[0, 0].astype(f32)
    inv = lax.rsqrt(jnp.mean(values * values, axis=-1, keepdims=True) + norm_eps)
    normed = (values * inv * gain_ref[...]).astype(bf16)
    cut_blocks(normed, h_ref)
    cut_blocks(stash_ref[0, 0], x_ref)
    inv_ref[...] = jnp.broadcast_to(inv, inv_ref.shape)


def split_kernel(now_ref, top_ref, gain_ref, now_out, top_out, gain_out):
    cut_blocks(now_ref[0], now_out)
    cut_blocks(top_ref[0], top_out)
    cut_blocks(gain_ref[...], gain_out)


def first_products(fsdp, left_ref, w_refs):
    total = None
    for j, w_ref in enumerate(w_refs):
        part = dot_nn(left_ref[lax.bitwise_xor(fsdp, j)], w_ref[...])
        total = part if total is None else total + part
    return total


def input_grad(fsdp, grad_pre, w_refs, x_ref, inv_ref, gain_ref, out_ref):
    inv = inv_ref[:, :1]
    moment = jnp.zeros((x_ref.shape[1], 1), f32)
    width = x_ref.shape[2]
    for j, w_ref in enumerate(w_refs):
        block = lax.bitwise_xor(fsdp, j)
        partial_dh = dot_nt(grad_pre, w_ref[...]).astype(bf16)
        scaled = x_ref[block].astype(f32) * inv
        gained = gain_ref[block] * partial_dh.astype(f32)
        moment += jnp.sum(gained * scaled, axis=-1, keepdims=True)
        out_ref[block, :, :width] = partial_dh
    high = moment.astype(bf16)
    low = (moment - high.astype(f32)).astype(bf16)
    rest = out_ref.shape[2] - width
    lane = lax.broadcasted_iota(jnp.int32, (x_ref.shape[1], rest), 1)
    tail = jnp.where(lane == 0, high.astype(f32), jnp.where(lane == 1, low.astype(f32), 0.0))
    for b in range(out_ref.shape[0]):
        out_ref[b, :, width:] = tail.astype(bf16)


def first_kernel(
    h_ref, dy_ref, w0, w1, w2, w3, x_ref, inv_ref, gain_ref, act_ref, pre_ref, out_ref
):
    fsdp = lax.axis_index("fsdp")
    w_refs = (w0, w1, w2, w3)
    hidden = first_products(fsdp, h_ref, w_refs)
    backed = first_products(fsdp, dy_ref, w_refs)
    activated, slope = gelu_and_slope(hidden)
    act_ref[...] = activated.astype(bf16)
    grad_pre = (slope * backed).astype(bf16)
    pre_ref[...] = grad_pre
    input_grad(fsdp, grad_pre, w_refs, x_ref, inv_ref, gain_ref, out_ref)


def ahead_kernel(h_ref, w0, w1, w2, w3, act_ref, slope_ref):
    fsdp = lax.axis_index("fsdp")
    activated, slope = gelu_and_slope(first_products(fsdp, h_ref, (w0, w1, w2, w3)))
    act_ref[...] = activated.astype(bf16)
    slope_ref[...] = slope


def second_kernel(
    slope_ref, got_ref, top_ref, w0, w1, w2, w3, x_ref, inv_ref, gain_ref, dy_ref, pre_ref, out_ref
):
    fsdp = lax.axis_index("fsdp")
    is_last = lax.axis_index("section") == lax.axis_size("section") - 1
    w_refs = (w0, w1, w2, w3)
    rows, width = got_ref.shape[1], x_ref.shape[2]

    @pl.when(is_last)
    def _():
        dy_ref[...] = top_ref[...]

    @pl.when(jnp.logical_not(is_last))
    def _():
        dy_ref[:, :rows] = got_ref[:, :, :width]
        dy_ref[:, rows:] = got_ref[:, :, width:]

    backed = first_products(fsdp, dy_ref, w_refs)
    grad_pre = (slope_ref[...] * backed).astype(bf16)
    pre_ref[...] = grad_pre
    input_grad(fsdp, grad_pre, w_refs, x_ref, inv_ref, gain_ref, out_ref)


def share_kernel(count, got_ref, x_ref, inv_ref, gain_ref, dy_ref, out_ref):
    tp = lax.axis_index("tp")
    width = x_ref.shape[2]
    inv = inv_ref[:, :1]
    total = got_ref[0, :, :width].astype(f32)
    tail = got_ref[0, :, width:].astype(f32)
    for b in range(1, got_ref.shape[0]):
        total += got_ref[b, :, :width].astype(f32)
        tail += got_ref[b, :, width:].astype(f32)
    mean = (tail[:, :1] + tail[:, 1:2]) / count
    scaled = x_ref[tp].astype(f32) * inv
    gained = gain_ref[tp] * total
    share = (dy_ref[tp].astype(f32) + inv * (gained - scaled * mean)).astype(bf16)
    rows = out_ref.shape[0]
    out_ref[:, :width] = share[:rows]
    out_ref[:, width:] = share[rows:]


def weight_grad_kernel(h_ref, dy_ref, pre_ref, act_ref, out_ref):
    fsdp = lax.axis_index("fsdp")
    for j in range(out_ref.shape[0]):
        block = lax.bitwise_xor(fsdp, j)
        out_ref[j] = dot_tn(h_ref[block], pre_ref[...]) + dot_tn(dy_ref[block], act_ref[...])


def weight_grad_end_kernel(h_ref, dy_ref, pre_ref, act_ref, acc_ref, keep_ref, send_ref):
    fsdp = lax.axis_index("fsdp")
    for j in range(acc_ref.shape[0]):
        block = lax.bitwise_xor(fsdp, j)
        total = (
            acc_ref[j] + dot_tn(h_ref[block], pre_ref[...]) + dot_tn(dy_ref[block], act_ref[...])
        )
        if j % 2:
            send_ref[j // 2] = total.astype(bf16)
        else:
            keep_ref[j // 2] = total


def last_kernel(got_ref, top_ref, out_ref):
    is_last = lax.axis_index("section") == lax.axis_size("section") - 1
    count, rows, width = got_ref.shape[0], got_ref.shape[1], got_ref.shape[2] // 2

    @pl.when(is_last)
    def _():
        out_ref[0] = top_ref[1]

    @pl.when(jnp.logical_not(is_last))
    def _():
        for b in range(count):
            out_ref[0, :rows, b * width : (b + 1) * width] = got_ref[b, :, :width]
            out_ref[0, rows:, b * width : (b + 1) * width] = got_ref[b, :, width:]


def swapped(values, axis, bit):
    return lax.ppermute(values, axis, [(i, i ^ bit) for i in range(lax.axis_size(axis))])


def moved_down(values):
    return lax.ppermute(
        values, "section", [(i, i - 1) for i in range(1, lax.axis_size("section"))]
    )


def exchanged(values):
    return lax.all_to_all(values, "tp", split_axis=0, concat_axis=0, tiled=True)


def copied_to_all(share):
    return exchanged(jnp.broadcast_to(share, (lax.axis_size("tp"), *share.shape)))


def per_device(stash, grad_now, grad_top, order, gain, weight):
    tp_count = lax.axis_size("tp")
    tokens, features = grad_now.shape[1:]
    width = features // tp_count
    inner = weight.shape[2]
    wide = -(-(width + 2) // 128) * 128
    ticks = grad_top.shape[0]
    sds = jax.ShapeDtypeStruct

    blocks = sds((tp_count, tokens, width), bf16)
    flat = sds((tokens, inner), bf16)
    sent = sds((tp_count, tokens, wide), bf16)
    share = sds((tokens // 2, 2 * width), bf16)
    own_share = functools.partial(share_kernel, features)
    dot = 2 * tokens * features * inner

    def prepared(tick):
        outs = [blocks, blocks, sds((tokens, 128), f32)]
        return pl.pallas_call(
            prepare_kernel,
            grid_spec=pltpu.PrefetchScalarGridSpec(
                num_scalar_prefetch=1,
                grid=(1,),
                in_specs=[
                    pl.BlockSpec((1, 1, tokens, features), lambda i, slot: (0, slot[0, tick], 0, 0)),
                    pl.BlockSpec((1, features), lambda i, slot: (0, 0)),
                ],
                out_specs=[
                    pl.BlockSpec(blocks.shape, lambda i, slot: (0, 0, 0)),
                    pl.BlockSpec(blocks.shape, lambda i, slot: (0, 0, 0)),
                    pl.BlockSpec((tokens, 128), lambda i, slot: (0, 0)),
                ],
            ),
            out_shape=outs,
            cost_estimate=cost(dot, outs, (gain,)),
            compiler_params=pltpu.CompilerParams(vmem_limit_bytes=vmem_budget),
        )(order, stash, gain)

    w0 = weight[0]
    w2 = swapped(w0, "fsdp", 2)
    w1 = swapped(w0, "fsdp", 1)
    h1, x1, inv1 = prepared(0)
    h2, x2, inv2 = prepared(1)
    dy1, top1, gains = call(
        split_kernel,
        dot,
        [blocks, blocks, sds((tp_count, 1, width), f32)],
        grad_now, grad_top, gain,
    )
    (w2, h1, x1, inv1, h2, x2, inv2, dy1, top1, gains) = lax.optimization_barrier(
        (w2, h1, x1, inv1, h2, x2, inv2, dy1, top1, gains)
    )
    w3 = swapped(w2, "fsdp", 1)
    weights = (w0, w1, w2, w3)

    act1, pre1, out1 = call(
        first_kernel, 3 * dot, [flat, flat, sent], h1, dy1, *weights, x1, inv1, gains
    )
    got1 = exchanged(out1)
    act2, slope2 = call(ahead_kernel, dot, [flat, sds((tokens, inner), f32)], h2, *weights)
    acc = call(
        weight_grad_kernel, 2 * dot, sds((tp_count, width, inner), f32), h1, dy1, pre1, act1
    )
    share1 = call(own_share, dot // 8, share, got1, x1, inv1, gains, dy1)
    held1 = copied_to_all(moved_down(share1))
    dy2, pre2, out2 = call(
        second_kernel,
        2 * dot,
        [blocks, flat, sent],
        slope2, held1, top1, *weights, x2, inv2, gains,
    )
    got2 = exchanged(out2)
    pair = (tp_count // 2, width, inner)
    keep, send = call(
        weight_grad_end_kernel,
        2 * dot,
        [sds(pair, f32), sds(pair, bf16)],
        h2, dy2, pre2, act2, acc,
    )
    from_core = swapped(send, "fsdp", 1)
    across = swapped((keep[1] + from_core[1].astype(f32)).astype(bf16), "fsdp", 2)
    weight_grad = keep[0] + from_core[0].astype(f32) + across.astype(f32)
    share2 = call(own_share, dot // 8, share, got2, x2, inv2, gains, dy2)
    held2 = copied_to_all(moved_down(share2))
    grad_held = call(last_kernel, dot // 8, sds((1, tokens, features), bf16), held2, grad_top)
    return (grad_held, weight_grad[None])


def solution(mesh):
    return jax.shard_map(
        per_device,
        mesh=mesh,
        in_specs=(
            P("section", None, "fsdp", None),
            P("section", "fsdp", None),
            P(None, "fsdp", None),
            P("section", None),
            P("section", None),
            P("section", "fsdp", "tp"),
        ),
        out_specs=(P("section", "fsdp", None), P("section", "fsdp", "tp")),
        check_vma=False,
    )
```

```python
import functools

import jax
import jax.numpy as jnp
from jax import lax
from jax.experimental import pallas as pl
from jax.experimental.pallas import tpu as pltpu
from jax.sharding import PartitionSpec as P


norm_eps = 1e-06
f32 = jnp.float32
bf16 = jnp.bfloat16
gelu_scale = 0.7978845608028654
gelu_cubic = 0.044715
vmem_budget = 16 * 1024 * 1024


def dot_nn(left, right):
    return jnp.dot(left, right, preferred_element_type=f32)


def dot_nt(left, right):
    return lax.dot_general(left, right, (((1,), (1,)), ((), ())), preferred_element_type=f32)


def dot_tn(left, right):
    return lax.dot_general(left, right, (((0,), (0,)), ((), ())), preferred_element_type=f32)


def gelu_and_slope(values):
    squared = values * values
    tanh = jnp.tanh(gelu_scale * values * (1.0 + gelu_cubic * squared))
    half = 0.5 * (1.0 + tanh)
    slope = half + 0.5 * values * (1.0 - tanh * tanh) * (
        gelu_scale * (1.0 + 3.0 * gelu_cubic * squared)
    )
    return values * half, slope


def cost(flops, outs, args):
    size = sum(v.size * v.dtype.itemsize for v in jax.tree.leaves((outs, args)))
    return pl.CostEstimate(flops=int(flops), bytes_accessed=size, transcendentals=0)


def call(kernel, flops, outs, *args):
    return pl.pallas_call(
        kernel,
        out_shape=outs,
        cost_estimate=cost(flops, outs, args),
        compiler_params=pltpu.CompilerParams(vmem_limit_bytes=vmem_budget),
    )(*args)


def cut_blocks(values, ref, first=0):
    count, width = ref.shape[0], ref.shape[2]
    rows = values.shape[0]
    for b in range(count):
        ref[b, first : first + rows] = values[:, b * width : (b + 1) * width]


def normalize(stash_ref, gain_ref, inv_ref):
    values = stash_ref[0, 0].astype(f32)
    inv = lax.rsqrt(jnp.mean(values * values, axis=-1, keepdims=True) + norm_eps)
    inv_ref[...] = jnp.broadcast_to(inv, inv_ref.shape)
    return (values * inv * gain_ref[...]).astype(bf16)


def prepare_first_kernel(order_ref, stash_ref, gain_ref, now_ref, left_ref, x_ref, inv_ref, gain_out):
    cut_blocks(normalize(stash_ref, gain_ref, inv_ref), left_ref)
    cut_blocks(now_ref[0], left_ref, now_ref.shape[1])
    cut_blocks(stash_ref[0, 0], x_ref)
    cut_blocks(gain_ref[...], gain_out)


def prepare_second_kernel(order_ref, stash_ref, gain_ref, top_ref, h_ref, x_ref, inv_ref, top_out):
    cut_blocks(normalize(stash_ref, gain_ref, inv_ref), h_ref)
    cut_blocks(stash_ref[0, 0], x_ref)
    cut_blocks(top_ref[0], top_out)


def first_products(fsdp, left_ref, w_refs):
    total = None
    for j, w_ref in enumerate(w_refs):
        part = dot_nn(left_ref[lax.bitwise_xor(fsdp, j)], w_ref[...])
        total = part if total is None else total + part
    return total


def input_grad(fsdp, grad_pre, w_refs, x_ref, inv_ref, gain_ref, out_ref):
    inv = inv_ref[:, :1]
    moment = jnp.zeros((x_ref.shape[1], 1), f32)
    width = x_ref.shape[2]
    for j, w_ref in enumerate(w_refs):
        block = lax.bitwise_xor(fsdp, j)
        partial_dh = dot_nt(grad_pre, w_ref[...]).astype(bf16)
        scaled = x_ref[block].astype(f32) * inv
        gained = gain_ref[block] * partial_dh.astype(f32)
        moment += jnp.sum(gained * scaled, axis=-1, keepdims=True)
        out_ref[block, :, :width] = partial_dh
    high = moment.astype(bf16)
    low = (moment - high.astype(f32)).astype(bf16)
    rest = out_ref.shape[2] - width
    lane = lax.broadcasted_iota(jnp.int32, (x_ref.shape[1], rest), 1)
    tail = jnp.where(lane == 0, high.astype(f32), jnp.where(lane == 1, low.astype(f32), 0.0))
    for b in range(out_ref.shape[0]):
        out_ref[b, :, width:] = tail.astype(bf16)


def first_kernel(
    left_ref, w0, w1, w2, w3, x_ref, inv_ref, gain_ref, right_ref, out_ref, x_own, dy_own
):
    fsdp = lax.axis_index("fsdp")
    tp = lax.axis_index("tp")
    rows = x_ref.shape[1]
    x_own[...] = x_ref[tp]
    dy_own[...] = left_ref[tp, rows:]
    w_refs = (w0, w1, w2, w3)
    products = first_products(fsdp, left_ref, w_refs)
    activated, slope = gelu_and_slope(products[:rows])
    grad_pre = (slope * products[rows:]).astype(bf16)
    right_ref[:rows] = grad_pre
    right_ref[rows:] = activated.astype(bf16)
    input_grad(fsdp, grad_pre, w_refs, x_ref, inv_ref, gain_ref, out_ref)


def between_kernel(left_ref, right_ref, h_ref, w0, w1, w2, w3, acc_ref, act_ref, slope_ref):
    fsdp = lax.axis_index("fsdp")
    activated, slope = gelu_and_slope(first_products(fsdp, h_ref, (w0, w1, w2, w3)))
    act_ref[...] = activated.astype(bf16)
    slope_ref[...] = slope
    for j in range(acc_ref.shape[0]):
        acc_ref[j] = dot_tn(left_ref[lax.bitwise_xor(fsdp, j)], right_ref[...])


def second_kernel(
    slope_ref, got_ref, top_ref, w0, w1, w2, w3, x_ref, inv_ref, gain_ref,
    dy_ref, pre_ref, out_ref, x_own, dy_own,
):
    fsdp = lax.axis_index("fsdp")
    tp = lax.axis_index("tp")
    is_last = lax.axis_index("section") == lax.axis_size("section") - 1
    w_refs = (w0, w1, w2, w3)
    rows, width = got_ref.shape[1], x_ref.shape[2]

    @pl.when(is_last)
    def _():
        dy_ref[...] = top_ref[...]

    @pl.when(jnp.logical_not(is_last))
    def _():
        dy_ref[:, :rows] = got_ref[:, :, :width]
        dy_ref[:, rows:] = got_ref[:, :, width:]

    x_own[...] = x_ref[tp]
    dy_own[...] = dy_ref[tp]
    backed = first_products(fsdp, dy_ref, w_refs)
    grad_pre = (slope_ref[...] * backed).astype(bf16)
    pre_ref[...] = grad_pre
    input_grad(fsdp, grad_pre, w_refs, x_ref, inv_ref, gain_ref, out_ref)


def share_kernel(count, got_ref, x_ref, inv_ref, gain_ref, dy_ref, out_ref):
    tp = lax.axis_index("tp")
    width = x_ref.shape[1]
    inv = inv_ref[:, :1]
    total = got_ref[0, :, :width].astype(f32)
    tail = got_ref[0, :, width:].astype(f32)
    for b in range(1, got_ref.shape[0]):
        total += got_ref[b, :, :width].astype(f32)
        tail += got_ref[b, :, width:].astype(f32)
    mean = (tail[:, :1] + tail[:, 1:2]) / count
    scaled = x_ref[...].astype(f32) * inv
    gained = gain_ref[tp] * total
    share = (dy_ref[...].astype(f32) + inv * (gained - scaled * mean)).astype(bf16)
    rows = out_ref.shape[0]
    out_ref[:, :width] = share[:rows]
    out_ref[:, width:] = share[rows:]


def late_kernel(h_ref, dy_ref, pre_ref, act_ref, acc_ref, keep_ref, send_ref):
    fsdp = lax.axis_index("fsdp")
    right = jnp.concatenate([pre_ref[...], act_ref[...]], axis=0)
    for j in range(acc_ref.shape[0]):
        block = lax.bitwise_xor(fsdp, j)
        left = jnp.concatenate([h_ref[block], dy_ref[block]], axis=0)
        total = acc_ref[j] + dot_tn(left, right)
        if j % 2:
            send_ref[j // 2] = total.astype(bf16)
        else:
            keep_ref[j // 2] = total


def last_kernel(got_ref, top_ref, out_ref):
    is_last = lax.axis_index("section") == lax.axis_size("section") - 1
    count, rows, width = got_ref.shape[0], got_ref.shape[1], got_ref.shape[2] // 2

    @pl.when(is_last)
    def _():
        out_ref[0] = top_ref[1]

    @pl.when(jnp.logical_not(is_last))
    def _():
        for b in range(count):
            out_ref[0, :rows, b * width : (b + 1) * width] = got_ref[b, :, :width]
            out_ref[0, rows:, b * width : (b + 1) * width] = got_ref[b, :, width:]


def swapped(values, axis, bit):
    return lax.ppermute(values, axis, [(i, i ^ bit) for i in range(lax.axis_size(axis))])


def moved_down(values):
    return lax.ppermute(
        values, "section", [(i, i - 1) for i in range(1, lax.axis_size("section"))]
    )


def exchanged(values):
    return lax.all_to_all(values, "tp", split_axis=0, concat_axis=0, tiled=True)


def copied_to_all(share):
    return exchanged(jnp.broadcast_to(share, (lax.axis_size("tp"), *share.shape)))


def per_device(stash, grad_now, grad_top, order, gain, weight):
    tp_count = lax.axis_size("tp")
    tokens, features = grad_now.shape[1:]
    width = features // tp_count
    inner = weight.shape[2]
    wide = -(-(width + 2) // 128) * 128
    sds = jax.ShapeDtypeStruct

    blocks = sds((tp_count, tokens, width), bf16)
    pairs = sds((tp_count, 2 * tokens, width), bf16)
    flat = sds((tokens, inner), bf16)
    sent = sds((tp_count, tokens, wide), bf16)
    own = [sds((tokens, width), bf16)] * 2
    share = sds((tokens // 2, 2 * width), bf16)
    stats = sds((tokens, 128), f32)
    gain_blocks = sds((tp_count, 1, width), f32)
    own_share = functools.partial(share_kernel, features)
    dot = 2 * tokens * features * inner

    def prepared(kernel, tick, extra, extra_shape, outs):
        whole = [pl.BlockSpec(v.shape, lambda i, slot, n=len(v.shape): (0,) * n) for v in outs]
        return pl.pallas_call(
            kernel,
            grid_spec=pltpu.PrefetchScalarGridSpec(
                num_scalar_prefetch=1,
                grid=(1,),
                in_specs=[
                    pl.BlockSpec((1, 1, tokens, features), lambda i, slot: (0, slot[0, tick], 0, 0)),
                    pl.BlockSpec((1, features), lambda i, slot: (0, 0)),
                    pl.BlockSpec(extra_shape, lambda i, slot: (0, 0, 0)),
                ],
                out_specs=whole,
            ),
            out_shape=outs,
            cost_estimate=cost(dot, outs, (gain,)),
            compiler_params=pltpu.CompilerParams(vmem_limit_bytes=vmem_budget),
        )(order, stash, gain, extra)

    w0 = weight[0]
    w2 = swapped(w0, "fsdp", 2)
    w1 = swapped(w0, "fsdp", 1)
    one = (1, tokens, features)
    left1, x1, inv1, gains = prepared(
        prepare_first_kernel, 0, grad_now, one, [pairs, blocks, stats, gain_blocks]
    )
    h2, x2, inv2, top1 = prepared(
        prepare_second_kernel, 1, grad_top, one, [blocks, blocks, stats, blocks]
    )
    (w2, left1, x1, inv1, gains, h2, x2, inv2, top1) = lax.optimization_barrier(
        (w2, left1, x1, inv1, gains, h2, x2, inv2, top1)
    )
    w3 = swapped(w2, "fsdp", 1)
    weights = (w0, w1, w2, w3)

    right1, out1, x1_own, dy1_own = call(
        first_kernel,
        3 * dot,
        [sds((2 * tokens, inner), bf16), sent, *own],
        left1, *weights, x1, inv1, gains,
    )
    got1 = exchanged(out1)
    share1 = call(own_share, dot // 8, share, got1, x1_own, inv1, gains, dy1_own)
    arrived1 = moved_down(share1)
    acc, act2, slope2 = call(
        between_kernel,
        3 * dot,
        [sds((tp_count, width, inner), f32), flat, sds((tokens, inner), f32)],
        left1, right1, h2, *weights,
    )
    (arrived1, acc, act2, slope2) = lax.optimization_barrier((arrived1, acc, act2, slope2))
    held1 = copied_to_all(arrived1)
    dy2, pre2, out2, x2_own, dy2_own = call(
        second_kernel,
        2 * dot,
        [blocks, flat, sent, *own],
        slope2, held1, top1, *weights, x2, inv2, gains,
    )
    pair = (tp_count // 2, width, inner)
    keep, send = call(
        late_kernel,
        2 * dot,
        [sds(pair, f32), sds(pair, bf16)],
        h2, dy2, pre2, act2, acc,
    )
    (out2, keep, send) = lax.optimization_barrier((out2, keep, send))
    got2 = exchanged(out2)
    share2 = call(own_share, dot // 8, share, got2, x2_own, inv2, gains, dy2_own)
    arrived2 = moved_down(share2)
    from_core = swapped(send, "fsdp", 1)
    across = swapped((keep[1] + from_core[1].astype(f32)).astype(bf16), "fsdp", 2)
    weight_grad = keep[0] + from_core[0].astype(f32) + across.astype(f32)
    held2 = copied_to_all(arrived2)
    grad_held = call(last_kernel, dot // 8, sds((1, tokens, features), bf16), held2, grad_top)
    return (grad_held, weight_grad[None])


def solution(mesh):
    return jax.shard_map(
        per_device,
        mesh=mesh,
        in_specs=(
            P("section", None, "fsdp", None),
            P("section", "fsdp", None),
            P(None, "fsdp", None),
            P("section", None),
            P("section", None),
            P("section", "fsdp", "tp"),
        ),
        out_specs=(P("section", "fsdp", None), P("section", "fsdp", "tp")),
        check_vma=False,
    )
```

```python
import functools

import jax
import jax.numpy as jnp
from jax import lax
from jax.experimental import pallas as pl
from jax.experimental.pallas import tpu as pltpu
from jax.sharding import PartitionSpec as P


norm_eps = 1e-06
f32 = jnp.float32
bf16 = jnp.bfloat16
gelu_scale = 0.7978845608028654
gelu_cubic = 0.044715
vmem_budget = 16 * 1024 * 1024


def dot_nn(left, right):
    return jnp.dot(left, right, preferred_element_type=f32)


def dot_nt(left, right):
    return lax.dot_general(left, right, (((1,), (1,)), ((), ())), preferred_element_type=f32)


def dot_tn(left, right):
    return lax.dot_general(left, right, (((0,), (0,)), ((), ())), preferred_element_type=f32)


def gelu_and_slope(values):
    squared = values * values
    tanh = jnp.tanh(gelu_scale * values * (1.0 + gelu_cubic * squared))
    half = 0.5 * (1.0 + tanh)
    slope = half + 0.5 * values * (1.0 - tanh * tanh) * (
        gelu_scale * (1.0 + 3.0 * gelu_cubic * squared)
    )
    return values * half, slope


def cost(flops, outs, args):
    size = sum(v.size * v.dtype.itemsize for v in jax.tree.leaves((outs, args)))
    return pl.CostEstimate(flops=int(flops), bytes_accessed=size, transcendentals=0)


def call(kernel, flops, outs, *args):
    return pl.pallas_call(
        kernel,
        out_shape=outs,
        cost_estimate=cost(flops, outs, args),
        compiler_params=pltpu.CompilerParams(vmem_limit_bytes=vmem_budget),
    )(*args)


def cut_blocks(values, ref, first=0):
    count, width = ref.shape[0], ref.shape[2]
    rows = values.shape[0]
    for b in range(count):
        ref[b, first : first + rows] = values[:, b * width : (b + 1) * width]


def normalize(stash_ref, gain_ref, inv_ref):
    values = stash_ref[0, 0].astype(f32)
    inv = lax.rsqrt(jnp.mean(values * values, axis=-1, keepdims=True) + norm_eps)
    inv_ref[...] = jnp.broadcast_to(inv, inv_ref.shape)
    return (values * inv * gain_ref[...]).astype(bf16)


def prepare_first_kernel(order_ref, stash_ref, gain_ref, now_ref, left_ref, x_ref, inv_ref, gain_out):
    cut_blocks(normalize(stash_ref, gain_ref, inv_ref), left_ref)
    cut_blocks(now_ref[0], left_ref, now_ref.shape[1])
    cut_blocks(stash_ref[0, 0], x_ref)
    cut_blocks(gain_ref[...], gain_out)


def prepare_second_kernel(order_ref, stash_ref, gain_ref, top_ref, h_ref, x_ref, inv_ref, top_out):
    cut_blocks(normalize(stash_ref, gain_ref, inv_ref), h_ref)
    cut_blocks(stash_ref[0, 0], x_ref)
    cut_blocks(top_ref[0], top_out)


def first_products(fsdp, left_ref, w_refs):
    total = None
    for j, w_ref in enumerate(w_refs):
        part = dot_nn(left_ref[lax.bitwise_xor(fsdp, j)], w_ref[...])
        total = part if total is None else total + part
    return total


def input_grad(fsdp, grad_pre, w_refs, x_ref, inv_ref, gain_ref, out_ref):
    inv = inv_ref[:, :1]
    moment = jnp.zeros((x_ref.shape[1], 1), f32)
    width = x_ref.shape[2]
    for j, w_ref in enumerate(w_refs):
        block = lax.bitwise_xor(fsdp, j)
        partial_dh = dot_nt(grad_pre, w_ref[...]).astype(bf16)
        scaled = x_ref[block].astype(f32) * inv
        gained = gain_ref[block] * partial_dh.astype(f32)
        moment += jnp.sum(gained * scaled, axis=-1, keepdims=True)
        out_ref[block, :, :width] = partial_dh
    high = moment.astype(bf16)
    low = (moment - high.astype(f32)).astype(bf16)
    rest = out_ref.shape[2] - width
    lane = lax.broadcasted_iota(jnp.int32, (x_ref.shape[1], rest), 1)
    tail = jnp.where(lane == 0, high.astype(f32), jnp.where(lane == 1, low.astype(f32), 0.0))
    for b in range(out_ref.shape[0]):
        out_ref[b, :, width:] = tail.astype(bf16)


def part_kernel(left_ref, w0, w1, w2, x_ref, part_ref, x_own, dy_own):
    tp = lax.axis_index("tp")
    x_own[...] = x_ref[tp]
    dy_own[...] = left_ref[tp, x_ref.shape[1] :]
    part_ref[...] = first_products(lax.axis_index("fsdp"), left_ref, (w0, w1, w2))


def first_kernel(
    part_ref, left_ref, w0, w1, w2, w3, x_ref, inv_ref, gain_ref, right_ref, out_ref
):
    fsdp = lax.axis_index("fsdp")
    rows = x_ref.shape[1]
    w_refs = (w0, w1, w2, w3)
    last = lax.bitwise_xor(fsdp, len(w_refs) - 1)
    products = part_ref[...] + dot_nn(left_ref[last], w3[...])
    activated, slope = gelu_and_slope(products[:rows])
    grad_pre = (slope * products[rows:]).astype(bf16)
    right_ref[:rows] = grad_pre
    right_ref[rows:] = activated.astype(bf16)
    input_grad(fsdp, grad_pre, w_refs, x_ref, inv_ref, gain_ref, out_ref)


def between_kernel(left_ref, right_ref, h_ref, w0, w1, w2, w3, acc_ref, act_ref, slope_ref):
    fsdp = lax.axis_index("fsdp")
    activated, slope = gelu_and_slope(first_products(fsdp, h_ref, (w0, w1, w2, w3)))
    act_ref[...] = activated.astype(bf16)
    slope_ref[...] = slope
    for j in range(acc_ref.shape[0]):
        acc_ref[j] = dot_tn(left_ref[lax.bitwise_xor(fsdp, j)], right_ref[...])


def second_kernel(
    slope_ref, got_ref, top_ref, w0, w1, w2, w3, x_ref, inv_ref, gain_ref,
    dy_ref, pre_ref, out_ref, x_own, dy_own,
):
    fsdp = lax.axis_index("fsdp")
    tp = lax.axis_index("tp")
    is_last = lax.axis_index("section") == lax.axis_size("section") - 1
    w_refs = (w0, w1, w2, w3)
    rows, width = got_ref.shape[1], x_ref.shape[2]

    @pl.when(is_last)
    def _():
        dy_ref[...] = top_ref[...]

    @pl.when(jnp.logical_not(is_last))
    def _():
        dy_ref[:, :rows] = got_ref[:, :, :width]
        dy_ref[:, rows:] = got_ref[:, :, width:]

    x_own[...] = x_ref[tp]
    dy_own[...] = dy_ref[tp]
    backed = first_products(fsdp, dy_ref, w_refs)
    grad_pre = (slope_ref[...] * backed).astype(bf16)
    pre_ref[...] = grad_pre
    input_grad(fsdp, grad_pre, w_refs, x_ref, inv_ref, gain_ref, out_ref)


def share_kernel(count, got_ref, x_ref, inv_ref, gain_ref, dy_ref, out_ref):
    tp = lax.axis_index("tp")
    width = x_ref.shape[1]
    inv = inv_ref[:, :1]
    total = got_ref[0, :, :width].astype(f32)
    tail = got_ref[0, :, width:].astype(f32)
    for b in range(1, got_ref.shape[0]):
        total += got_ref[b, :, :width].astype(f32)
        tail += got_ref[b, :, width:].astype(f32)
    mean = (tail[:, :1] + tail[:, 1:2]) / count
    scaled = x_ref[...].astype(f32) * inv
    gained = gain_ref[tp] * total
    share = (dy_ref[...].astype(f32) + inv * (gained - scaled * mean)).astype(bf16)
    rows = out_ref.shape[0]
    out_ref[:, :width] = share[:rows]
    out_ref[:, width:] = share[rows:]


def late_kernel(h_ref, dy_ref, pre_ref, act_ref, acc_ref, keep_ref, send_ref):
    fsdp = lax.axis_index("fsdp")
    right = jnp.concatenate([pre_ref[...], act_ref[...]], axis=0)
    for j in range(acc_ref.shape[0]):
        block = lax.bitwise_xor(fsdp, j)
        left = jnp.concatenate([h_ref[block], dy_ref[block]], axis=0)
        total = acc_ref[j] + dot_tn(left, right)
        if j % 2:
            send_ref[j // 2] = total.astype(bf16)
        else:
            keep_ref[j // 2] = total


def last_kernel(got_ref, top_ref, keep_ref, core_ref, across_ref, held_ref, grad_ref):
    is_last = lax.axis_index("section") == lax.axis_size("section") - 1
    step = pl.program_id(0)
    count, half_rows, width = got_ref.shape[0], got_ref.shape[1], got_ref.shape[2] // 2
    rows = held_ref.shape[1]
    per_half = half_rows // rows

    @pl.when(is_last)
    def _():
        held_ref[...] = top_ref[...]

    for half in range(2):

        @pl.when(jnp.logical_not(is_last) & (step // per_half == half))
        def _():
            start = pl.multiple_of(lax.rem(step, per_half) * rows, rows)
            for b in range(count):
                held_ref[0, :, b * width : (b + 1) * width] = got_ref[
                    b, pl.ds(start, rows), half * width : (half + 1) * width
                ]

    grad_ref[0] = keep_ref[0] + core_ref[0].astype(f32) + across_ref[...].astype(f32)


def swapped(values, axis, bit):
    return lax.ppermute(values, axis, [(i, i ^ bit) for i in range(lax.axis_size(axis))])


def moved_down(values):
    return lax.ppermute(
        values, "section", [(i, i - 1) for i in range(1, lax.axis_size("section"))]
    )


def exchanged(values):
    return lax.all_to_all(values, "tp", split_axis=0, concat_axis=0, tiled=True)


def copied_to_all(share):
    return exchanged(jnp.broadcast_to(share, (lax.axis_size("tp"), *share.shape)))


def per_device(stash, grad_now, grad_top, order, gain, weight):
    tp_count = lax.axis_size("tp")
    tokens, features = grad_now.shape[1:]
    width = features // tp_count
    inner = weight.shape[2]
    wide = -(-(width + 2) // 128) * 128
    sds = jax.ShapeDtypeStruct

    blocks = sds((tp_count, tokens, width), bf16)
    pairs = sds((tp_count, 2 * tokens, width), bf16)
    flat = sds((tokens, inner), bf16)
    sent = sds((tp_count, tokens, wide), bf16)
    own = [sds((tokens, width), bf16)] * 2
    share = sds((tokens // 2, 2 * width), bf16)
    stats = sds((tokens, 128), f32)
    gain_blocks = sds((tp_count, 1, width), f32)
    own_share = functools.partial(share_kernel, features)
    dot = 2 * tokens * features * inner

    def prepared(kernel, tick, extra, extra_shape, outs):
        whole = [pl.BlockSpec(v.shape, lambda i, slot, n=len(v.shape): (0,) * n) for v in outs]
        return pl.pallas_call(
            kernel,
            grid_spec=pltpu.PrefetchScalarGridSpec(
                num_scalar_prefetch=1,
                grid=(1,),
                in_specs=[
                    pl.BlockSpec((1, 1, tokens, features), lambda i, slot: (0, slot[0, tick], 0, 0)),
                    pl.BlockSpec((1, features), lambda i, slot: (0, 0)),
                    pl.BlockSpec(extra_shape, lambda i, slot: (0, 0, 0)),
                ],
                out_specs=whole,
            ),
            out_shape=outs,
            cost_estimate=cost(dot, outs, (gain,)),
            compiler_params=pltpu.CompilerParams(vmem_limit_bytes=vmem_budget),
        )(order, stash, gain, extra)

    w0 = weight[0]
    w2 = swapped(w0, "fsdp", 2)
    w1 = swapped(w0, "fsdp", 1)
    one = (1, tokens, features)
    left1, x1, inv1, gains = prepared(
        prepare_first_kernel, 0, grad_now, one, [pairs, blocks, stats, gain_blocks]
    )
    h2, x2, inv2, top1 = prepared(
        prepare_second_kernel, 1, grad_top, one, [blocks, blocks, stats, blocks]
    )
    (w2, left1, x1, inv1, gains, h2, x2, inv2, top1) = lax.optimization_barrier(
        (w2, left1, x1, inv1, gains, h2, x2, inv2, top1)
    )
    w3 = swapped(w2, "fsdp", 1)
    weights = (w0, w1, w2, w3)

    part1, x1_own, dy1_own = call(
        part_kernel,
        dot,
        [sds((2 * tokens, inner), f32), *own],
        left1, w0, w1, w2, x1,
    )
    right1, out1 = call(
        first_kernel,
        2 * dot,
        [sds((2 * tokens, inner), bf16), sent],
        part1, left1, *weights, x1, inv1, gains,
    )
    got1 = exchanged(out1)
    share1 = call(own_share, dot // 8, share, got1, x1_own, inv1, gains, dy1_own)
    arrived1 = moved_down(share1)
    acc, act2, slope2 = call(
        between_kernel,
        3 * dot,
        [sds((tp_count, width, inner), f32), flat, sds((tokens, inner), f32)],
        left1, right1, h2, *weights,
    )
    (arrived1, acc, act2, slope2) = lax.optimization_barrier((arrived1, acc, act2, slope2))
    held1 = copied_to_all(arrived1)
    dy2, pre2, out2, x2_own, dy2_own = call(
        second_kernel,
        2 * dot,
        [blocks, flat, sent, *own],
        slope2, held1, top1, *weights, x2, inv2, gains,
    )
    pair = (tp_count // 2, width, inner)
    keep, send = call(
        late_kernel,
        2 * dot,
        [sds(pair, f32), sds(pair, bf16)],
        h2, dy2, pre2, act2, acc,
    )
    from_core = swapped(send, "fsdp", 1)
    got2 = exchanged(out2)
    share2 = call(own_share, dot // 8, share, got2, x2_own, inv2, gains, dy2_own)
    arrived2 = moved_down(share2)
    across = keep[1] + from_core[1].astype(f32)
    across = swapped(across.astype(bf16), "fsdp", 2)
    held2 = copied_to_all(arrived2)
    steps = 4
    grad_rows = width // steps
    grad_held, weight_grad = pl.pallas_call(
        last_kernel,
        grid=(steps,),
        in_specs=[
            pl.BlockSpec(held2.shape, lambda i: (0, 0, 0)),
            pl.BlockSpec((1, tokens // steps, features), lambda i: (1, i, 0)),
            pl.BlockSpec((1, grad_rows, inner), lambda i: (0, i, 0)),
            pl.BlockSpec((1, grad_rows, inner), lambda i: (0, i, 0)),
            pl.BlockSpec((grad_rows, inner), lambda i: (i, 0)),
        ],
        out_specs=[
            pl.BlockSpec((1, tokens // steps, features), lambda i: (0, i, 0)),
            pl.BlockSpec((1, grad_rows, inner), lambda i: (0, i, 0)),
        ],
        out_shape=[sds((1, tokens, features), bf16), sds((1, width, inner), f32)],
        compiler_params=pltpu.CompilerParams(vmem_limit_bytes=vmem_budget),
    )(held2, grad_top, keep, from_core, across)
    return (grad_held, weight_grad)


def solution(mesh):
    return jax.shard_map(
        per_device,
        mesh=mesh,
        in_specs=(
            P("section", None, "fsdp", None),
            P("section", "fsdp", None),
            P(None, "fsdp", None),
            P("section", None),
            P("section", None),
            P("section", "fsdp", "tp"),
        ),
        out_specs=(P("section", "fsdp", None), P("section", "fsdp", "tp")),
        check_vma=False,
    )
```

```python
import functools

import jax
import jax.numpy as jnp
from jax import lax
from jax.experimental import pallas as pl
from jax.experimental.pallas import tpu as pltpu
from jax.sharding import PartitionSpec as P


norm_eps = 1e-06
f32 = jnp.float32
bf16 = jnp.bfloat16
gelu_scale = 0.7978845608028654
gelu_cubic = 0.044715
vmem_budget = 16 * 1024 * 1024


def dot_nn(left, right):
    return jnp.dot(left, right, preferred_element_type=f32)


def dot_nt(left, right):
    return lax.dot_general(left, right, (((1,), (1,)), ((), ())), preferred_element_type=f32)


def dot_tn(left, right):
    return lax.dot_general(left, right, (((0,), (0,)), ((), ())), preferred_element_type=f32)


def gelu_and_slope(values):
    squared = values * values
    tanh = jnp.tanh(gelu_scale * values * (1.0 + gelu_cubic * squared))
    half = 0.5 * (1.0 + tanh)
    slope = half + 0.5 * values * (1.0 - tanh * tanh) * (
        gelu_scale * (1.0 + 3.0 * gelu_cubic * squared)
    )
    return values * half, slope


def cost(flops, outs, args):
    size = sum(v.size * v.dtype.itemsize for v in jax.tree.leaves((outs, args)))
    return pl.CostEstimate(flops=int(flops), bytes_accessed=size, transcendentals=0)


def call(kernel, flops, outs, *args):
    return pl.pallas_call(
        kernel,
        out_shape=outs,
        cost_estimate=cost(flops, outs, args),
        compiler_params=pltpu.CompilerParams(vmem_limit_bytes=vmem_budget),
    )(*args)


def cut_blocks(values, ref, first=0):
    count, width = ref.shape[0], ref.shape[2]
    rows = values.shape[0]
    for b in range(count):
        ref[b, first : first + rows] = values[:, b * width : (b + 1) * width]


def normalize(stash_ref, gain_ref, inv_ref):
    values = stash_ref[0, 0].astype(f32)
    inv = lax.rsqrt(jnp.mean(values * values, axis=-1, keepdims=True) + norm_eps)
    inv_ref[...] = jnp.broadcast_to(inv, inv_ref.shape)
    return (values * inv * gain_ref[...]).astype(bf16)


def own_block(values, ref):
    width = ref.shape[1]
    for b in range(values.shape[1] // width):

        @pl.when(lax.axis_index("tp") == b)
        def _():
            ref[...] = values[:, b * width : (b + 1) * width]


def prepare_first_kernel(
    order_ref, stash_ref, gain_ref, now_ref, left_ref, x_own, inv_ref, dy_own, gain_out
):
    cut_blocks(normalize(stash_ref, gain_ref, inv_ref), left_ref)
    cut_blocks(now_ref[0], left_ref, now_ref.shape[1])
    own_block(stash_ref[0, 0], x_own)
    own_block(now_ref[0], dy_own)
    own_block(gain_ref[...], gain_out)


def prepare_second_kernel(order_ref, stash_ref, gain_ref, top_ref, h_ref, x_own, inv_ref, top_out):
    cut_blocks(normalize(stash_ref, gain_ref, inv_ref), h_ref)
    own_block(stash_ref[0, 0], x_own)
    cut_blocks(top_ref[0], top_out)


def first_products(fsdp, left_ref, w_refs):
    total = None
    for j, w_ref in enumerate(w_refs):
        part = dot_nn(left_ref[lax.bitwise_xor(fsdp, j)], w_ref[...])
        total = part if total is None else total + part
    return total


def input_grad(fsdp, hidden, grad_pre, w_refs, width, out_ref):
    for j, w_ref in enumerate(w_refs):
        out_ref[lax.bitwise_xor(fsdp, j), :, :width] = dot_nt(grad_pre, w_ref[...]).astype(bf16)
    moment = jnp.sum(hidden * grad_pre.astype(f32), axis=-1, keepdims=True)
    high = moment.astype(bf16)
    low = (moment - high.astype(f32)).astype(bf16)
    rest = out_ref.shape[2] - width
    lane = lax.broadcasted_iota(jnp.int32, (out_ref.shape[1], rest), 1)
    tail = jnp.where(lane == 0, high.astype(f32), jnp.where(lane == 1, low.astype(f32), 0.0))
    for b in range(out_ref.shape[0]):
        out_ref[b, :, width:] = tail.astype(bf16)


def part_kernel(left_ref, w0, w1, w2, part_ref):
    part_ref[...] = first_products(lax.axis_index("fsdp"), left_ref, (w0, w1, w2))


def first_kernel(part_ref, left_ref, w0, w1, w2, w3, right_ref, out_ref):
    fsdp = lax.axis_index("fsdp")
    rows = out_ref.shape[1]
    w_refs = (w0, w1, w2, w3)
    last = lax.bitwise_xor(fsdp, len(w_refs) - 1)
    products = part_ref[...] + dot_nn(left_ref[last], w3[...])
    hidden = products[:rows]
    activated, slope = gelu_and_slope(hidden)
    grad_pre = (slope * products[rows:]).astype(bf16)
    right_ref[:rows] = grad_pre
    right_ref[rows:] = activated.astype(bf16)
    input_grad(fsdp, hidden, grad_pre, w_refs, left_ref.shape[2], out_ref)


def between_kernel(
    left_ref, right_ref, h_ref, w0, w1, w2, w3, acc_ref, act_ref, hidden_ref, slope_ref
):
    fsdp = lax.axis_index("fsdp")
    hidden = first_products(fsdp, h_ref, (w0, w1, w2, w3))
    activated, slope = gelu_and_slope(hidden)
    act_ref[...] = activated.astype(bf16)
    hidden_ref[...] = hidden
    slope_ref[...] = slope
    for j in range(acc_ref.shape[0]):
        acc_ref[j] = dot_tn(left_ref[lax.bitwise_xor(fsdp, j)], right_ref[...])


def second_kernel(
    hidden_ref, slope_ref, got_ref, top_ref, w0, w1, w2, w3, dy_ref, pre_ref, out_ref, dy_own
):
    fsdp = lax.axis_index("fsdp")
    is_last = lax.axis_index("section") == lax.axis_size("section") - 1
    w_refs = (w0, w1, w2, w3)
    rows, width = got_ref.shape[1], dy_ref.shape[2]

    @pl.when(is_last)
    def _():
        dy_ref[...] = top_ref[...]

    @pl.when(jnp.logical_not(is_last))
    def _():
        dy_ref[:, :rows] = got_ref[:, :, :width]
        dy_ref[:, rows:] = got_ref[:, :, width:]

    dy_own[...] = dy_ref[lax.axis_index("tp")]
    backed = first_products(fsdp, dy_ref, w_refs)
    grad_pre = (slope_ref[...] * backed).astype(bf16)
    pre_ref[...] = grad_pre
    input_grad(fsdp, hidden_ref[...], grad_pre, w_refs, width, out_ref)


def share_kernel(count, got_ref, x_ref, inv_ref, gain_ref, dy_ref, out_ref):
    width = x_ref.shape[1]
    inv = inv_ref[:, :1]
    total = got_ref[0, :, :width].astype(f32)
    tail = got_ref[0, :, width:].astype(f32)
    for b in range(1, got_ref.shape[0]):
        total += got_ref[b, :, :width].astype(f32)
        tail += got_ref[b, :, width:].astype(f32)
    mean = (tail[:, :1] + tail[:, 1:2]) / count
    scaled = x_ref[...].astype(f32) * inv
    gained = gain_ref[...] * total
    share = (dy_ref[...].astype(f32) + inv * (gained - scaled * mean)).astype(bf16)
    rows = out_ref.shape[0]
    out_ref[:, :width] = share[:rows]
    out_ref[:, width:] = share[rows:]


def late_kernel(h_ref, dy_ref, pre_ref, act_ref, acc_ref, keep_ref, send_ref):
    fsdp = lax.axis_index("fsdp")
    right = jnp.concatenate([pre_ref[...], act_ref[...]], axis=0)
    for j in range(acc_ref.shape[0]):
        block = lax.bitwise_xor(fsdp, j)
        left = jnp.concatenate([h_ref[block], dy_ref[block]], axis=0)
        total = acc_ref[j] + dot_tn(left, right)
        if j % 2:
            send_ref[j // 2] = total.astype(bf16)
        else:
            keep_ref[j // 2] = total


def last_kernel(got_ref, top_ref, keep_ref, core_ref, across_ref, held_ref, grad_ref):
    is_last = lax.axis_index("section") == lax.axis_size("section") - 1
    step = pl.program_id(0)
    count, half_rows, width = got_ref.shape[0], got_ref.shape[1], got_ref.shape[2] // 2
    rows = held_ref.shape[1]
    per_half = half_rows // rows

    @pl.when(is_last)
    def _():
        held_ref[...] = top_ref[...]

    for half in range(2):

        @pl.when(jnp.logical_not(is_last) & (step // per_half == half))
        def _():
            start = pl.multiple_of(lax.rem(step, per_half) * rows, rows)
            for b in range(count):
                held_ref[0, :, b * width : (b + 1) * width] = got_ref[
                    b, pl.ds(start, rows), half * width : (half + 1) * width
                ]

    grad_ref[0] = keep_ref[0] + core_ref[0].astype(f32) + across_ref[...].astype(f32)


def swapped(values, axis, bit):
    return lax.ppermute(values, axis, [(i, i ^ bit) for i in range(lax.axis_size(axis))])


def moved_down(values):
    return lax.ppermute(
        values, "section", [(i, i - 1) for i in range(1, lax.axis_size("section"))]
    )


def exchanged(values):
    return lax.all_to_all(values, "tp", split_axis=0, concat_axis=0, tiled=True)


def copied_to_all(share):
    return exchanged(jnp.broadcast_to(share, (lax.axis_size("tp"), *share.shape)))


def per_device(stash, grad_now, grad_top, order, gain, weight):
    tp_count = lax.axis_size("tp")
    tokens, features = grad_now.shape[1:]
    width = features // tp_count
    inner = weight.shape[2]
    wide = -(-(width + 2) // 128) * 128
    sds = jax.ShapeDtypeStruct

    blocks = sds((tp_count, tokens, width), bf16)
    pairs = sds((tp_count, 2 * tokens, width), bf16)
    flat = sds((tokens, inner), bf16)
    sent = sds((tp_count, tokens, wide), bf16)
    own = sds((tokens, width), bf16)
    share = sds((tokens // 2, 2 * width), bf16)
    stats = sds((tokens, 128), f32)
    gain_own = sds((1, width), f32)
    high = sds((tokens, inner), f32)
    own_share = functools.partial(share_kernel, features)
    dot = 2 * tokens * features * inner

    def prepared(kernel, tick, extra, extra_shape, outs):
        whole = [pl.BlockSpec(v.shape, lambda i, slot, n=len(v.shape): (0,) * n) for v in outs]
        return pl.pallas_call(
            kernel,
            grid_spec=pltpu.PrefetchScalarGridSpec(
                num_scalar_prefetch=1,
                grid=(1,),
                in_specs=[
                    pl.BlockSpec((1, 1, tokens, features), lambda i, slot: (0, slot[0, tick], 0, 0)),
                    pl.BlockSpec((1, features), lambda i, slot: (0, 0)),
                    pl.BlockSpec(extra_shape, lambda i, slot: (0, 0, 0)),
                ],
                out_specs=whole,
            ),
            out_shape=outs,
            cost_estimate=cost(dot, outs, (gain,)),
            compiler_params=pltpu.CompilerParams(vmem_limit_bytes=vmem_budget),
        )(order, stash, gain, extra)

    w0 = weight[0]
    w2 = swapped(w0, "fsdp", 2)
    w1 = swapped(w0, "fsdp", 1)
    one = (1, tokens, features)
    left1, x1, inv1, dy1, gains = prepared(
        prepare_first_kernel, 0, grad_now, one, [pairs, own, stats, own, gain_own]
    )
    h2, x2, inv2, top1 = prepared(
        prepare_second_kernel, 1, grad_top, one, [blocks, own, stats, blocks]
    )
    (w2, left1, x1, inv1, dy1, gains, h2, x2, inv2, top1) = lax.optimization_barrier(
        (w2, left1, x1, inv1, dy1, gains, h2, x2, inv2, top1)
    )
    w3 = swapped(w2, "fsdp", 1)
    weights = (w0, w1, w2, w3)

    part1 = call(part_kernel, dot, sds((2 * tokens, inner), f32), left1, w0, w1, w2)
    right1, out1 = call(
        first_kernel, 2 * dot, [sds((2 * tokens, inner), bf16), sent], part1, left1, *weights
    )
    got1 = exchanged(out1)
    share1 = call(own_share, dot // 8, share, got1, x1, inv1, gains, dy1)
    arrived1 = moved_down(share1)
    acc, act2, hidden2, slope2 = call(
        between_kernel,
        3 * dot,
        [sds((tp_count, width, inner), f32), flat, high, high],
        left1, right1, h2, *weights,
    )
    (arrived1, acc, act2, hidden2, slope2) = lax.optimization_barrier(
        (arrived1, acc, act2, hidden2, slope2)
    )
    held1 = copied_to_all(arrived1)
    dy2, pre2, out2, dy2_own = call(
        second_kernel,
        2 * dot,
        [blocks, flat, sent, own],
        hidden2, slope2, held1, top1, *weights,
    )
    pair = (tp_count // 2, width, inner)
    keep, send = call(
        late_kernel,
        2 * dot,
        [sds(pair, f32), sds(pair, bf16)],
        h2, dy2, pre2, act2, acc,
    )
    (out2, keep, send) = lax.optimization_barrier((out2, keep, send))
    got2 = exchanged(out2)
    share2 = call(own_share, dot // 8, share, got2, x2, inv2, gains, dy2_own)
    arrived2 = moved_down(share2)
    from_core = swapped(send, "fsdp", 1)
    across = keep[1] + from_core[1].astype(f32)
    across = swapped(across.astype(bf16), "fsdp", 2)
    held2 = copied_to_all(arrived2)
    steps = 4
    grad_rows = width // steps
    grad_held, weight_grad = pl.pallas_call(
        last_kernel,
        grid=(steps,),
        in_specs=[
            pl.BlockSpec(held2.shape, lambda i: (0, 0, 0)),
            pl.BlockSpec((1, tokens // steps, features), lambda i: (1, i, 0)),
            pl.BlockSpec((1, grad_rows, inner), lambda i: (0, i, 0)),
            pl.BlockSpec((1, grad_rows, inner), lambda i: (0, i, 0)),
            pl.BlockSpec((grad_rows, inner), lambda i: (i, 0)),
        ],
        out_specs=[
            pl.BlockSpec((1, tokens // steps, features), lambda i: (0, i, 0)),
            pl.BlockSpec((1, grad_rows, inner), lambda i: (0, i, 0)),
        ],
        out_shape=[sds((1, tokens, features), bf16), sds((1, width, inner), f32)],
        compiler_params=pltpu.CompilerParams(vmem_limit_bytes=vmem_budget),
    )(held2, grad_top, keep, from_core, across)
    return (grad_held, weight_grad)


def solution(mesh):
    return jax.shard_map(
        per_device,
        mesh=mesh,
        in_specs=(
            P("section", None, "fsdp", None),
            P("section", "fsdp", None),
            P(None, "fsdp", None),
            P("section", None),
            P("section", None),
            P("section", "fsdp", "tp"),
        ),
        out_specs=(P("section", "fsdp", None), P("section", "fsdp", "tp")),
        check_vma=False,
    )
```

```python
import functools

import jax
import jax.numpy as jnp
from jax import lax
from jax.experimental import pallas as pl
from jax.experimental.pallas import tpu as pltpu
from jax.sharding import PartitionSpec as P


norm_eps = 1e-06
f32 = jnp.float32
bf16 = jnp.bfloat16
gelu_scale = 0.7978845608028654
gelu_cubic = 0.044715
vmem_budget = 16 * 1024 * 1024


def dot_nn(left, right):
    return jnp.dot(left, right, preferred_element_type=f32)


def dot_nt(left, right):
    return lax.dot_general(left, right, (((1,), (1,)), ((), ())), preferred_element_type=f32)


def dot_tn(left, right):
    return lax.dot_general(left, right, (((0,), (0,)), ((), ())), preferred_element_type=f32)


def gelu_and_slope(values):
    squared = values * values
    tanh = jnp.tanh(gelu_scale * values * (1.0 + gelu_cubic * squared))
    half = 0.5 * (1.0 + tanh)
    slope = half + 0.5 * values * (1.0 - tanh * tanh) * (
        gelu_scale * (1.0 + 3.0 * gelu_cubic * squared)
    )
    return values * half, slope


def cost(flops, outs, args):
    size = sum(v.size * v.dtype.itemsize for v in jax.tree.leaves((outs, args)))
    return pl.CostEstimate(flops=int(flops), bytes_accessed=size, transcendentals=0)


def call(kernel, flops, outs, *args):
    return pl.pallas_call(
        kernel,
        out_shape=outs,
        cost_estimate=cost(flops, outs, args),
        compiler_params=pltpu.CompilerParams(vmem_limit_bytes=vmem_budget),
    )(*args)


def cut_blocks(values, ref, first=0):
    count, width = ref.shape[0], ref.shape[2]
    rows = values.shape[0]
    for b in range(count):
        ref[b, first : first + rows] = values[:, b * width : (b + 1) * width]


def normalize(stash_ref, gain_ref, inv_ref):
    values = stash_ref[0, 0].astype(f32)
    inv = lax.rsqrt(jnp.mean(values * values, axis=-1, keepdims=True) + norm_eps)
    inv_ref[...] = jnp.broadcast_to(inv, inv_ref.shape)
    return (values * inv * gain_ref[...]).astype(bf16)


def own_block(values, ref):
    width = ref.shape[1]
    for b in range(values.shape[1] // width):

        @pl.when(lax.axis_index("tp") == b)
        def _():
            ref[...] = values[:, b * width : (b + 1) * width]


def prepare_first_kernel(
    order_ref, stash_ref, gain_ref, now_ref, left_ref, x_own, inv_ref, dy_own, gain_out
):
    cut_blocks(normalize(stash_ref, gain_ref, inv_ref), left_ref)
    cut_blocks(now_ref[0], left_ref, now_ref.shape[1])
    own_block(stash_ref[0, 0], x_own)
    own_block(now_ref[0], dy_own)
    own_block(gain_ref[...], gain_out)


def prepare_second_kernel(order_ref, stash_ref, gain_ref, top_ref, h_ref, x_own, inv_ref, top_out):
    cut_blocks(normalize(stash_ref, gain_ref, inv_ref), h_ref)
    own_block(stash_ref[0, 0], x_own)
    cut_blocks(top_ref[0], top_out)


def first_products(fsdp, left_ref, w_refs):
    total = None
    for j, w_ref in enumerate(w_refs):
        part = dot_nn(left_ref[lax.bitwise_xor(fsdp, j)], w_ref[...])
        total = part if total is None else total + part
    return total


def input_grad(fsdp, hidden, grad_pre, w_refs, width, out_ref):
    for j, w_ref in enumerate(w_refs):
        out_ref[lax.bitwise_xor(fsdp, j), :, :width] = dot_nt(grad_pre, w_ref[...]).astype(bf16)
    moment = jnp.sum(hidden * grad_pre.astype(f32), axis=-1, keepdims=True)
    high = moment.astype(bf16)
    low = (moment - high.astype(f32)).astype(bf16)
    rest = out_ref.shape[2] - width
    lane = lax.broadcasted_iota(jnp.int32, (out_ref.shape[1], rest), 1)
    tail = jnp.where(lane == 0, high.astype(f32), jnp.where(lane == 1, low.astype(f32), 0.0))
    for b in range(out_ref.shape[0]):
        out_ref[b, :, width:] = tail.astype(bf16)


def part_kernel(left_ref, w0, w1, w2, part_ref):
    part_ref[...] = first_products(lax.axis_index("fsdp"), left_ref, (w0, w1, w2))


def first_kernel(part_ref, left_ref, w0, w1, w2, w3, right_ref, out_ref):
    fsdp = lax.axis_index("fsdp")
    rows = out_ref.shape[1]
    w_refs = (w0, w1, w2, w3)
    last = lax.bitwise_xor(fsdp, len(w_refs) - 1)
    products = part_ref[...] + dot_nn(left_ref[last], w3[...])
    hidden = products[:rows]
    activated, slope = gelu_and_slope(hidden)
    grad_pre = (slope * products[rows:]).astype(bf16)
    right_ref[:rows] = grad_pre
    right_ref[rows:] = activated.astype(bf16)
    input_grad(fsdp, hidden, grad_pre, w_refs, left_ref.shape[2], out_ref)


def between_kernel(
    left_ref, right_ref, h_ref, w0, w1, w2, w3, acc_ref, act_ref, hidden_ref, slope_ref
):
    fsdp = lax.axis_index("fsdp")
    hidden = first_products(fsdp, h_ref, (w0, w1, w2, w3))
    activated, slope = gelu_and_slope(hidden)
    act_ref[...] = activated.astype(bf16)
    hidden_ref[...] = hidden
    slope_ref[...] = slope
    for j in range(acc_ref.shape[0]):
        acc_ref[j] = dot_tn(left_ref[lax.bitwise_xor(fsdp, j)], right_ref[...])


def second_kernel(
    hidden_ref, slope_ref, got_ref, top_ref, w0, w1, w2, w3, dy_ref, pre_ref, out_ref, dy_own
):
    fsdp = lax.axis_index("fsdp")
    is_last = lax.axis_index("section") == lax.axis_size("section") - 1
    w_refs = (w0, w1, w2, w3)
    rows, width = got_ref.shape[1], dy_ref.shape[2]

    @pl.when(is_last)
    def _():
        dy_ref[...] = top_ref[...]

    @pl.when(jnp.logical_not(is_last))
    def _():
        dy_ref[:, :rows] = got_ref[:, :, :width]
        dy_ref[:, rows:] = got_ref[:, :, width:]

    dy_own[...] = dy_ref[lax.axis_index("tp")]
    backed = first_products(fsdp, dy_ref, w_refs)
    grad_pre = (slope_ref[...] * backed).astype(bf16)
    pre_ref[...] = grad_pre
    input_grad(fsdp, hidden_ref[...], grad_pre, w_refs, width, out_ref)


def share_kernel(count, got_ref, x_ref, inv_ref, gain_ref, dy_ref, out_ref):
    width = x_ref.shape[1]
    inv = inv_ref[:, :1]
    total = got_ref[0, :, :width].astype(f32)
    tail = got_ref[0, :, width:].astype(f32)
    for b in range(1, got_ref.shape[0]):
        total += got_ref[b, :, :width].astype(f32)
        tail += got_ref[b, :, width:].astype(f32)
    mean = (tail[:, :1] + tail[:, 1:2]) / count
    scaled = x_ref[...].astype(f32) * inv
    gained = gain_ref[...] * total
    share = (dy_ref[...].astype(f32) + inv * (gained - scaled * mean)).astype(bf16)
    rows = out_ref.shape[0]
    out_ref[:, :width] = share[:rows]
    out_ref[:, width:] = share[rows:]


def late_kernel(h_ref, dy_ref, pre_ref, act_ref, acc_ref, keep_ref, send_ref):
    fsdp = lax.axis_index("fsdp")
    right = jnp.concatenate([pre_ref[...], act_ref[...]], axis=0)
    for j in range(acc_ref.shape[0]):
        block = lax.bitwise_xor(fsdp, j)
        left = jnp.concatenate([h_ref[block], dy_ref[block]], axis=0)
        total = acc_ref[j] + dot_tn(left, right)
        if j % 2:
            send_ref[j // 2] = total.astype(bf16)
        else:
            keep_ref[j // 2] = total


def last_kernel(got_ref, top_ref, held_ref):
    is_last = lax.axis_index("section") == lax.axis_size("section") - 1
    count, rows, width = got_ref.shape[0], got_ref.shape[1], got_ref.shape[2] // 2

    @pl.when(is_last)
    def _():
        held_ref[0] = top_ref[1]

    @pl.when(jnp.logical_not(is_last))
    def _():
        for b in range(count):
            held_ref[0, :rows, b * width : (b + 1) * width] = got_ref[b, :, :width]
            held_ref[0, rows:, b * width : (b + 1) * width] = got_ref[b, :, width:]


def join_kernel(keep_ref, core_ref, across_ref, grad_ref):
    grad_ref[0] = keep_ref[0] + core_ref[0].astype(f32) + across_ref[...].astype(f32)


def swapped(values, axis, bit):
    return lax.ppermute(values, axis, [(i, i ^ bit) for i in range(lax.axis_size(axis))])


def moved_down(values):
    return lax.ppermute(
        values, "section", [(i, i - 1) for i in range(1, lax.axis_size("section"))]
    )


def exchanged(values):
    return lax.all_to_all(values, "tp", split_axis=0, concat_axis=0, tiled=True)


def copied_to_all(share):
    return exchanged(jnp.broadcast_to(share, (lax.axis_size("tp"), *share.shape)))


def per_device(stash, grad_now, grad_top, order, gain, weight):
    tp_count = lax.axis_size("tp")
    tokens, features = grad_now.shape[1:]
    width = features // tp_count
    inner = weight.shape[2]
    wide = -(-(width + 2) // 128) * 128
    sds = jax.ShapeDtypeStruct

    blocks = sds((tp_count, tokens, width), bf16)
    pairs = sds((tp_count, 2 * tokens, width), bf16)
    flat = sds((tokens, inner), bf16)
    sent = sds((tp_count, tokens, wide), bf16)
    own = sds((tokens, width), bf16)
    share = sds((tokens // 2, 2 * width), bf16)
    stats = sds((tokens, 128), f32)
    gain_own = sds((1, width), f32)
    high = sds((tokens, inner), f32)
    own_share = functools.partial(share_kernel, features)
    dot = 2 * tokens * features * inner

    def prepared(kernel, tick, extra, extra_shape, outs):
        whole = [pl.BlockSpec(v.shape, lambda i, slot, n=len(v.shape): (0,) * n) for v in outs]
        return pl.pallas_call(
            kernel,
            grid_spec=pltpu.PrefetchScalarGridSpec(
                num_scalar_prefetch=1,
                grid=(1,),
                in_specs=[
                    pl.BlockSpec((1, 1, tokens, features), lambda i, slot: (0, slot[0, tick], 0, 0)),
                    pl.BlockSpec((1, features), lambda i, slot: (0, 0)),
                    pl.BlockSpec(extra_shape, lambda i, slot: (0, 0, 0)),
                ],
                out_specs=whole,
            ),
            out_shape=outs,
            cost_estimate=cost(dot, outs, (gain,)),
            compiler_params=pltpu.CompilerParams(vmem_limit_bytes=vmem_budget),
        )(order, stash, gain, extra)

    w0 = weight[0]
    w2 = swapped(w0, "fsdp", 2)
    w1 = swapped(w0, "fsdp", 1)
    one = (1, tokens, features)
    left1, x1, inv1, dy1, gains = prepared(
        prepare_first_kernel, 0, grad_now, one, [pairs, own, stats, own, gain_own]
    )
    h2, x2, inv2, top1 = prepared(
        prepare_second_kernel, 1, grad_top, one, [blocks, own, stats, blocks]
    )
    (w2, left1, x1, inv1, dy1, gains, h2, x2, inv2, top1) = lax.optimization_barrier(
        (w2, left1, x1, inv1, dy1, gains, h2, x2, inv2, top1)
    )
    w3 = swapped(w2, "fsdp", 1)
    weights = (w0, w1, w2, w3)

    part1 = call(part_kernel, dot, sds((2 * tokens, inner), f32), left1, w0, w1, w2)
    right1, out1 = call(
        first_kernel, 2 * dot, [sds((2 * tokens, inner), bf16), sent], part1, left1, *weights
    )
    got1 = exchanged(out1)
    share1 = call(own_share, dot // 8, share, got1, x1, inv1, gains, dy1)
    arrived1 = moved_down(share1)
    acc, act2, hidden2, slope2 = call(
        between_kernel,
        3 * dot,
        [sds((tp_count, width, inner), f32), flat, high, high],
        left1, right1, h2, *weights,
    )
    (arrived1, acc, act2, hidden2, slope2) = lax.optimization_barrier(
        (arrived1, acc, act2, hidden2, slope2)
    )
    held1 = copied_to_all(arrived1)
    dy2, pre2, out2, dy2_own = call(
        second_kernel,
        2 * dot,
        [blocks, flat, sent, own],
        hidden2, slope2, held1, top1, *weights,
    )
    pair = (tp_count // 2, width, inner)
    keep, send = call(
        late_kernel,
        2 * dot,
        [sds(pair, f32), sds(pair, bf16)],
        h2, dy2, pre2, act2, acc,
    )
    (out2, keep, send) = lax.optimization_barrier((out2, keep, send))
    got2 = exchanged(out2)
    share2 = call(own_share, dot // 8, share, got2, x2, inv2, gains, dy2_own)
    arrived2 = moved_down(share2)
    from_core = swapped(send, "fsdp", 1)
    across = keep[1] + from_core[1].astype(f32)
    across = swapped(across.astype(bf16), "fsdp", 2)
    held2 = copied_to_all(arrived2)
    grad_held = call(last_kernel, dot // 8, sds((1, tokens, features), bf16), held2, grad_top)
    steps = 3
    grad_rows = width // steps
    weight_grad = pl.pallas_call(
        join_kernel,
        grid=(steps,),
        in_specs=[
            pl.BlockSpec((1, grad_rows, inner), lambda i: (0, i, 0)),
            pl.BlockSpec((1, grad_rows, inner), lambda i: (0, i, 0)),
            pl.BlockSpec((grad_rows, inner), lambda i: (i, 0)),
        ],
        out_specs=pl.BlockSpec((1, grad_rows, inner), lambda i: (0, i, 0)),
        out_shape=sds((1, width, inner), f32),
        compiler_params=pltpu.CompilerParams(vmem_limit_bytes=vmem_budget),
    )(keep, from_core, across)
    return (grad_held, weight_grad)


def solution(mesh):
    return jax.shard_map(
        per_device,
        mesh=mesh,
        in_specs=(
            P("section", None, "fsdp", None),
            P("section", "fsdp", None),
            P(None, "fsdp", None),
            P("section", None),
            P("section", None),
            P("section", "fsdp", "tp"),
        ),
        out_specs=(P("section", "fsdp", None), P("section", "fsdp", "tp")),
        check_vma=False,
    )
```

```python
import functools

import jax
import jax.numpy as jnp
from jax import lax
from jax.experimental import pallas as pl
from jax.experimental.pallas import tpu as pltpu
from jax.sharding import PartitionSpec as P


norm_eps = 1e-06
f32 = jnp.float32
bf16 = jnp.bfloat16
gelu_scale = 0.7978845608028654
gelu_cubic = 0.044715
vmem_budget = 16 * 1024 * 1024


def dot_nn(left, right):
    return jnp.dot(left, right, preferred_element_type=f32)


def dot_nt(left, right):
    return lax.dot_general(left, right, (((1,), (1,)), ((), ())), preferred_element_type=f32)


def dot_tn(left, right):
    return lax.dot_general(left, right, (((0,), (0,)), ((), ())), preferred_element_type=f32)


def gelu_and_slope(values):
    squared = values * values
    tanh = jnp.tanh(gelu_scale * values * (1.0 + gelu_cubic * squared))
    half = 0.5 * (1.0 + tanh)
    slope = half + 0.5 * values * (1.0 - tanh * tanh) * (
        gelu_scale * (1.0 + 3.0 * gelu_cubic * squared)
    )
    return values * half, slope


def cost(flops, outs, args):
    size = sum(v.size * v.dtype.itemsize for v in jax.tree.leaves((outs, args)))
    return pl.CostEstimate(flops=int(flops), bytes_accessed=size, transcendentals=0)


def call(kernel, flops, outs, *args):
    return pl.pallas_call(
        kernel,
        out_shape=outs,
        cost_estimate=cost(flops, outs, args),
        compiler_params=pltpu.CompilerParams(vmem_limit_bytes=vmem_budget),
    )(*args)


def cut_blocks(values, ref, first=0):
    count, width = ref.shape[0], ref.shape[2]
    rows = values.shape[0]
    for b in range(count):
        ref[b, first : first + rows] = values[:, b * width : (b + 1) * width]


def normalize(stash_ref, gain_ref, inv_ref):
    values = stash_ref[0, 0].astype(f32)
    inv = lax.rsqrt(jnp.mean(values * values, axis=-1, keepdims=True) + norm_eps)
    inv_ref[...] = jnp.broadcast_to(inv, inv_ref.shape)
    return (values * inv * gain_ref[...]).astype(bf16)


def own_block(values, ref):
    width = ref.shape[1]
    for b in range(values.shape[1] // width):

        @pl.when(lax.axis_index("tp") == b)
        def _():
            ref[...] = values[:, b * width : (b + 1) * width]


def prepare_first_kernel(
    order_ref, stash_ref, gain_ref, now_ref, left_ref, x_own, inv_ref, dy_own, gain_out
):
    cut_blocks(normalize(stash_ref, gain_ref, inv_ref), left_ref)
    cut_blocks(now_ref[0], left_ref, now_ref.shape[1])
    own_block(stash_ref[0, 0], x_own)
    own_block(now_ref[0], dy_own)
    own_block(gain_ref[...], gain_out)


def prepare_second_kernel(order_ref, stash_ref, gain_ref, top_ref, h_ref, x_own, inv_ref, top_out):
    cut_blocks(normalize(stash_ref, gain_ref, inv_ref), h_ref)
    own_block(stash_ref[0, 0], x_own)
    cut_blocks(top_ref[0], top_out)


def first_products(fsdp, left_ref, w_refs):
    total = None
    for j, w_ref in enumerate(w_refs):
        part = dot_nn(left_ref[lax.bitwise_xor(fsdp, j)], w_ref[...])
        total = part if total is None else total + part
    return total


def input_grad(fsdp, hidden, grad_pre, w_refs, width, out_ref):
    for j, w_ref in enumerate(w_refs):
        out_ref[lax.bitwise_xor(fsdp, j), :, :width] = dot_nt(grad_pre, w_ref[...]).astype(bf16)
    moment = jnp.sum(hidden * grad_pre.astype(f32), axis=-1, keepdims=True)
    high = moment.astype(bf16)
    low = (moment - high.astype(f32)).astype(bf16)
    rest = out_ref.shape[2] - width
    lane = lax.broadcasted_iota(jnp.int32, (out_ref.shape[1], rest), 1)
    tail = jnp.where(lane == 0, high.astype(f32), jnp.where(lane == 1, low.astype(f32), 0.0))
    for b in range(out_ref.shape[0]):
        out_ref[b, :, width:] = tail.astype(bf16)


def part_kernel(left_ref, w0, w1, w2, part_ref):
    part_ref[...] = first_products(lax.axis_index("fsdp"), left_ref, (w0, w1, w2))


def first_kernel(part_ref, left_ref, w0, w1, w2, w3, right_ref, out_ref):
    fsdp = lax.axis_index("fsdp")
    rows = out_ref.shape[1]
    w_refs = (w0, w1, w2, w3)
    last = lax.bitwise_xor(fsdp, len(w_refs) - 1)
    products = part_ref[...] + dot_nn(left_ref[last], w3[...])
    hidden = products[:rows]
    activated, slope = gelu_and_slope(hidden)
    grad_pre = (slope * products[rows:]).astype(bf16)
    right_ref[:rows] = grad_pre
    right_ref[rows:] = activated.astype(bf16)
    input_grad(fsdp, hidden, grad_pre, w_refs, left_ref.shape[2], out_ref)


def between_kernel(
    left_ref, right_ref, h_ref, w0, w1, w2, w3, acc_ref, act_ref, hidden_ref, slope_ref
):
    fsdp = lax.axis_index("fsdp")
    hidden = first_products(fsdp, h_ref, (w0, w1, w2, w3))
    activated, slope = gelu_and_slope(hidden)
    act_ref[...] = activated.astype(bf16)
    hidden_ref[...] = hidden
    slope_ref[...] = slope
    for j in range(acc_ref.shape[0]):
        acc_ref[j] = dot_tn(left_ref[lax.bitwise_xor(fsdp, j)], right_ref[...])


def second_kernel(
    hidden_ref, slope_ref, got_ref, top_ref, w0, w1, w2, w3, dy_ref, pre_ref, out_ref, dy_own
):
    fsdp = lax.axis_index("fsdp")
    is_last = lax.axis_index("section") == lax.axis_size("section") - 1
    w_refs = (w0, w1, w2, w3)
    rows, width = got_ref.shape[1], dy_ref.shape[2]

    @pl.when(is_last)
    def _():
        dy_ref[...] = top_ref[...]

    @pl.when(jnp.logical_not(is_last))
    def _():
        dy_ref[:, :rows] = got_ref[:, :, :width]
        dy_ref[:, rows:] = got_ref[:, :, width:]

    dy_own[...] = dy_ref[lax.axis_index("tp")]
    backed = first_products(fsdp, dy_ref, w_refs)
    grad_pre = (slope_ref[...] * backed).astype(bf16)
    pre_ref[...] = grad_pre
    input_grad(fsdp, hidden_ref[...], grad_pre, w_refs, width, out_ref)


def share_kernel(count, got_ref, x_ref, inv_ref, gain_ref, dy_ref, out_ref):
    width = x_ref.shape[1]
    inv = inv_ref[:, :1]
    total = got_ref[0, :, :width].astype(f32)
    tail = got_ref[0, :, width:].astype(f32)
    for b in range(1, got_ref.shape[0]):
        total += got_ref[b, :, :width].astype(f32)
        tail += got_ref[b, :, width:].astype(f32)
    mean = (tail[:, :1] + tail[:, 1:2]) / count
    scaled = x_ref[...].astype(f32) * inv
    gained = gain_ref[...] * total
    share = (dy_ref[...].astype(f32) + inv * (gained - scaled * mean)).astype(bf16)
    rows = out_ref.shape[0]
    out_ref[:, :width] = share[:rows]
    out_ref[:, width:] = share[rows:]


def late_kernel(h_ref, dy_ref, pre_ref, act_ref, acc_ref, keep_ref, send_ref):
    fsdp = lax.axis_index("fsdp")
    right = jnp.concatenate([pre_ref[...], act_ref[...]], axis=0)
    for j in range(acc_ref.shape[0]):
        block = lax.bitwise_xor(fsdp, j)
        left = jnp.concatenate([h_ref[block], dy_ref[block]], axis=0)
        total = acc_ref[j] + dot_tn(left, right)
        if j % 2:
            send_ref[j // 2] = total.astype(bf16)
        else:
            keep_ref[j // 2] = total


def last_kernel(got_ref, top_ref, held_ref):
    is_last = lax.axis_index("section") == lax.axis_size("section") - 1
    count, rows, width = got_ref.shape[0], got_ref.shape[1], got_ref.shape[2] // 2

    @pl.when(is_last)
    def _():
        held_ref[0] = top_ref[1]

    @pl.when(jnp.logical_not(is_last))
    def _():
        for b in range(count):
            held_ref[0, :rows, b * width : (b + 1) * width] = got_ref[b, :, :width]
            held_ref[0, rows:, b * width : (b + 1) * width] = got_ref[b, :, width:]


def swapped(values, axis, bit):
    return lax.ppermute(values, axis, [(i, i ^ bit) for i in range(lax.axis_size(axis))])


def moved_down(values):
    return lax.ppermute(
        values, "section", [(i, i - 1) for i in range(1, lax.axis_size("section"))]
    )


def exchanged(values):
    return lax.all_to_all(values, "tp", split_axis=0, concat_axis=0, tiled=True)


def copied_to_all(share):
    return exchanged(jnp.broadcast_to(share, (lax.axis_size("tp"), *share.shape)))


def per_device(stash, grad_now, grad_top, order, gain, weight):
    tp_count = lax.axis_size("tp")
    tokens, features = grad_now.shape[1:]
    width = features // tp_count
    inner = weight.shape[2]
    wide = -(-(width + 2) // 128) * 128
    sds = jax.ShapeDtypeStruct

    blocks = sds((tp_count, tokens, width), bf16)
    pairs = sds((tp_count, 2 * tokens, width), bf16)
    flat = sds((tokens, inner), bf16)
    sent = sds((tp_count, tokens, wide), bf16)
    own = sds((tokens, width), bf16)
    share = sds((tokens // 2, 2 * width), bf16)
    stats = sds((tokens, 128), f32)
    gain_own = sds((1, width), f32)
    high = sds((tokens, inner), f32)
    own_share = functools.partial(share_kernel, features)
    dot = 2 * tokens * features * inner

    def prepared(kernel, tick, extra, extra_shape, outs):
        whole = [pl.BlockSpec(v.shape, lambda i, slot, n=len(v.shape): (0,) * n) for v in outs]
        return pl.pallas_call(
            kernel,
            grid_spec=pltpu.PrefetchScalarGridSpec(
                num_scalar_prefetch=1,
                grid=(1,),
                in_specs=[
                    pl.BlockSpec((1, 1, tokens, features), lambda i, slot: (0, slot[0, tick], 0, 0)),
                    pl.BlockSpec((1, features), lambda i, slot: (0, 0)),
                    pl.BlockSpec(extra_shape, lambda i, slot: (0, 0, 0)),
                ],
                out_specs=whole,
            ),
            out_shape=outs,
            cost_estimate=cost(dot, outs, (gain,)),
            compiler_params=pltpu.CompilerParams(vmem_limit_bytes=vmem_budget),
        )(order, stash, gain, extra)

    w0 = weight[0]
    w2 = swapped(w0, "fsdp", 2)
    w1 = swapped(w0, "fsdp", 1)
    one = (1, tokens, features)
    left1, x1, inv1, dy1, gains = prepared(
        prepare_first_kernel, 0, grad_now, one, [pairs, own, stats, own, gain_own]
    )
    h2, x2, inv2, top1 = prepared(
        prepare_second_kernel, 1, grad_top, one, [blocks, own, stats, blocks]
    )
    (w2, left1, x1, inv1, dy1, gains, h2, x2, inv2, top1) = lax.optimization_barrier(
        (w2, left1, x1, inv1, dy1, gains, h2, x2, inv2, top1)
    )
    w3 = swapped(w2, "fsdp", 1)
    weights = (w0, w1, w2, w3)

    part1 = call(part_kernel, dot, sds((2 * tokens, inner), f32), left1, w0, w1, w2)
    right1, out1 = call(
        first_kernel, 2 * dot, [sds((2 * tokens, inner), bf16), sent], part1, left1, *weights
    )
    got1 = exchanged(out1)
    share1 = call(own_share, dot // 8, share, got1, x1, inv1, gains, dy1)
    arrived1 = moved_down(share1)
    acc, act2, hidden2, slope2 = call(
        between_kernel,
        3 * dot,
        [sds((tp_count, width, inner), f32), flat, high, high],
        left1, right1, h2, *weights,
    )
    (arrived1, acc, act2, hidden2, slope2) = lax.optimization_barrier(
        (arrived1, acc, act2, hidden2, slope2)
    )
    held1 = copied_to_all(arrived1)
    dy2, pre2, out2, dy2_own = call(
        second_kernel,
        2 * dot,
        [blocks, flat, sent, own],
        hidden2, slope2, held1, top1, *weights,
    )
    got2 = exchanged(out2)
    share2 = call(own_share, dot // 8, share, got2, x2, inv2, gains, dy2_own)
    arrived2 = moved_down(share2)
    pair = (tp_count // 2, width, inner)
    keep, send = call(
        late_kernel,
        2 * dot,
        [sds(pair, f32), sds(pair, bf16)],
        h2, dy2, pre2, act2, acc,
    )
    from_core = swapped(send, "fsdp", 1)
    across = keep[1] + from_core[1].astype(f32)
    across = swapped(across.astype(bf16), "fsdp", 2)
    held2 = copied_to_all(arrived2)
    grad_held = call(last_kernel, dot // 8, sds((1, tokens, features), bf16), held2, grad_top)
    weight_grad = keep[0] + from_core[0].astype(f32) + across.astype(f32)
    return (grad_held, weight_grad[None])


def solution(mesh):
    return jax.shard_map(
        per_device,
        mesh=mesh,
        in_specs=(
            P("section", None, "fsdp", None),
            P("section", "fsdp", None),
            P(None, "fsdp", None),
            P("section", None),
            P("section", None),
            P("section", "fsdp", "tp"),
        ),
        out_specs=(P("section", "fsdp", None), P("section", "fsdp", "tp")),
        check_vma=False,
    )
```

```python
import functools

import jax
import jax.numpy as jnp
from jax import lax
from jax.experimental import pallas as pl
from jax.experimental.pallas import tpu as pltpu
from jax.sharding import PartitionSpec as P


norm_eps = 1e-06
f32 = jnp.float32
bf16 = jnp.bfloat16
gelu_scale = 0.7978845608028654
gelu_cubic = 0.044715
vmem_budget = 16 * 1024 * 1024


def dot_nn(left, right):
    return jnp.dot(left, right, preferred_element_type=f32)


def dot_nt(left, right):
    return lax.dot_general(left, right, (((1,), (1,)), ((), ())), preferred_element_type=f32)


def dot_tn(left, right):
    return lax.dot_general(left, right, (((0,), (0,)), ((), ())), preferred_element_type=f32)


def gelu_and_slope(values):
    squared = values * values
    tanh = jnp.tanh(gelu_scale * values * (1.0 + gelu_cubic * squared))
    half = 0.5 * (1.0 + tanh)
    slope = half + 0.5 * values * (1.0 - tanh * tanh) * (
        gelu_scale * (1.0 + 3.0 * gelu_cubic * squared)
    )
    return values * half, slope


def cost(flops, outs, args):
    size = sum(v.size * v.dtype.itemsize for v in jax.tree.leaves((outs, args)))
    return pl.CostEstimate(flops=int(flops), bytes_accessed=size, transcendentals=0)


def call(kernel, flops, outs, *args):
    return pl.pallas_call(
        kernel,
        out_shape=outs,
        cost_estimate=cost(flops, outs, args),
        compiler_params=pltpu.CompilerParams(vmem_limit_bytes=vmem_budget),
    )(*args)


def cut_blocks(values, ref, first=0):
    count, width = ref.shape[0], ref.shape[2]
    rows = values.shape[0]
    for b in range(count):
        ref[b, first : first + rows] = values[:, b * width : (b + 1) * width]


def normalize(stash_ref, gain_ref, inv_ref):
    values = stash_ref[0, 0].astype(f32)
    inv = lax.rsqrt(jnp.mean(values * values, axis=-1, keepdims=True) + norm_eps)
    inv_ref[...] = jnp.broadcast_to(inv, inv_ref.shape)
    return (values * inv * gain_ref[...]).astype(bf16)


def own_block(values, ref):
    width = ref.shape[1]
    for b in range(values.shape[1] // width):

        @pl.when(lax.axis_index("tp") == b)
        def _():
            ref[...] = values[:, b * width : (b + 1) * width]


def prepare_first_kernel(
    order_ref, stash_ref, gain_ref, now_ref, left_ref, x_own, inv_ref, dy_own, gain_out
):
    cut_blocks(normalize(stash_ref, gain_ref, inv_ref), left_ref)
    cut_blocks(now_ref[0], left_ref, now_ref.shape[1])
    own_block(stash_ref[0, 0], x_own)
    own_block(now_ref[0], dy_own)
    own_block(gain_ref[...], gain_out)


def prepare_second_kernel(order_ref, stash_ref, gain_ref, top_ref, h_ref, x_own, inv_ref, top_out):
    cut_blocks(normalize(stash_ref, gain_ref, inv_ref), h_ref)
    own_block(stash_ref[0, 0], x_own)
    cut_blocks(top_ref[0], top_out)


def first_products(fsdp, left_ref, w_refs):
    total = None
    for j, w_ref in enumerate(w_refs):
        part = dot_nn(left_ref[lax.bitwise_xor(fsdp, j)], w_ref[...])
        total = part if total is None else total + part
    return total


def input_grad(fsdp, hidden, grad_pre, w_refs, width, out_ref):
    for j, w_ref in enumerate(w_refs):
        out_ref[lax.bitwise_xor(fsdp, j), :, :width] = dot_nt(grad_pre, w_ref[...]).astype(bf16)
    moment = jnp.sum(hidden * grad_pre.astype(f32), axis=-1, keepdims=True)
    high = moment.astype(bf16)
    low = (moment - high.astype(f32)).astype(bf16)
    rest = out_ref.shape[2] - width
    lane = lax.broadcasted_iota(jnp.int32, (out_ref.shape[1], rest), 1)
    tail = jnp.where(lane == 0, high.astype(f32), jnp.where(lane == 1, low.astype(f32), 0.0))
    for b in range(out_ref.shape[0]):
        out_ref[b, :, width:] = tail.astype(bf16)


def part_kernel(left_ref, w0, w1, w2, part_ref):
    part_ref[...] = first_products(lax.axis_index("fsdp"), left_ref, (w0, w1, w2))


def first_kernel(part_ref, left_ref, w0, w1, w2, w3, right_ref, out_ref):
    fsdp = lax.axis_index("fsdp")
    rows = out_ref.shape[1]
    w_refs = (w0, w1, w2, w3)
    last = lax.bitwise_xor(fsdp, len(w_refs) - 1)
    products = part_ref[...] + dot_nn(left_ref[last], w3[...])
    hidden = products[:rows]
    activated, slope = gelu_and_slope(hidden)
    grad_pre = (slope * products[rows:]).astype(bf16)
    right_ref[:rows] = grad_pre
    right_ref[rows:] = activated.astype(bf16)
    input_grad(fsdp, hidden, grad_pre, w_refs, left_ref.shape[2], out_ref)


def between_kernel(
    left_ref, right_ref, h_ref, w0, w1, w2, w3, acc_ref, act_ref, hidden_ref, slope_ref
):
    fsdp = lax.axis_index("fsdp")
    hidden = first_products(fsdp, h_ref, (w0, w1, w2, w3))
    activated, slope = gelu_and_slope(hidden)
    act_ref[...] = activated.astype(bf16)
    hidden_ref[...] = hidden
    slope_ref[...] = slope
    for n in range(acc_ref.shape[0]):
        acc_ref[n] = dot_tn(left_ref[lax.bitwise_xor(fsdp, 2 * n + 1)], right_ref[...])


def second_kernel(
    hidden_ref, slope_ref, got_ref, top_ref, w0, w1, w2, w3, dy_ref, pre_ref, out_ref, dy_own
):
    fsdp = lax.axis_index("fsdp")
    is_last = lax.axis_index("section") == lax.axis_size("section") - 1
    w_refs = (w0, w1, w2, w3)
    rows, width = got_ref.shape[1], dy_ref.shape[2]

    @pl.when(is_last)
    def _():
        dy_ref[...] = top_ref[...]

    @pl.when(jnp.logical_not(is_last))
    def _():
        dy_ref[:, :rows] = got_ref[:, :, :width]
        dy_ref[:, rows:] = got_ref[:, :, width:]

    dy_own[...] = dy_ref[lax.axis_index("tp")]
    backed = first_products(fsdp, dy_ref, w_refs)
    grad_pre = (slope_ref[...] * backed).astype(bf16)
    pre_ref[...] = grad_pre
    input_grad(fsdp, hidden_ref[...], grad_pre, w_refs, width, out_ref)


def share_kernel(count, got_ref, x_ref, inv_ref, gain_ref, dy_ref, out_ref):
    width = x_ref.shape[1]
    inv = inv_ref[:, :1]
    total = got_ref[0, :, :width].astype(f32)
    tail = got_ref[0, :, width:].astype(f32)
    for b in range(1, got_ref.shape[0]):
        total += got_ref[b, :, :width].astype(f32)
        tail += got_ref[b, :, width:].astype(f32)
    mean = (tail[:, :1] + tail[:, 1:2]) / count
    scaled = x_ref[...].astype(f32) * inv
    gained = gain_ref[...] * total
    share = (dy_ref[...].astype(f32) + inv * (gained - scaled * mean)).astype(bf16)
    rows = out_ref.shape[0]
    out_ref[:, :width] = share[:rows]
    out_ref[:, width:] = share[rows:]


def late_kernel(h_ref, dy_ref, pre_ref, act_ref, acc_ref, send_ref):
    fsdp = lax.axis_index("fsdp")
    right = jnp.concatenate([pre_ref[...], act_ref[...]], axis=0)
    for n in range(send_ref.shape[0]):
        block = lax.bitwise_xor(fsdp, 2 * n + 1)
        left = jnp.concatenate([h_ref[block], dy_ref[block]], axis=0)
        send_ref[n] = (acc_ref[n] + dot_tn(left, right)).astype(bf16)


def stay_kernel(left_ref, right_ref, h_ref, dy_ref, pre_ref, act_ref, keep_ref):
    fsdp = lax.axis_index("fsdp")
    right = jnp.concatenate([pre_ref[...], act_ref[...]], axis=0)
    for n in range(keep_ref.shape[0]):
        block = lax.bitwise_xor(fsdp, 2 * n)
        left = jnp.concatenate([h_ref[block], dy_ref[block]], axis=0)
        keep_ref[n] = dot_tn(left_ref[block], right_ref[...]) + dot_tn(left, right)


def last_kernel(got_ref, top_ref, held_ref):
    is_last = lax.axis_index("section") == lax.axis_size("section") - 1
    count, rows, width = got_ref.shape[0], got_ref.shape[1], got_ref.shape[2] // 2

    @pl.when(is_last)
    def _():
        held_ref[0] = top_ref[1]

    @pl.when(jnp.logical_not(is_last))
    def _():
        for b in range(count):
            held_ref[0, :rows, b * width : (b + 1) * width] = got_ref[b, :, :width]
            held_ref[0, rows:, b * width : (b + 1) * width] = got_ref[b, :, width:]


def swapped(values, axis, bit):
    return lax.ppermute(values, axis, [(i, i ^ bit) for i in range(lax.axis_size(axis))])


def moved_down(values):
    return lax.ppermute(
        values, "section", [(i, i - 1) for i in range(1, lax.axis_size("section"))]
    )


def exchanged(values):
    return lax.all_to_all(values, "tp", split_axis=0, concat_axis=0, tiled=True)


def copied_to_all(share):
    return exchanged(jnp.broadcast_to(share, (lax.axis_size("tp"), *share.shape)))


def per_device(stash, grad_now, grad_top, order, gain, weight):
    tp_count = lax.axis_size("tp")
    tokens, features = grad_now.shape[1:]
    width = features // tp_count
    inner = weight.shape[2]
    wide = -(-(width + 2) // 128) * 128
    sds = jax.ShapeDtypeStruct

    blocks = sds((tp_count, tokens, width), bf16)
    pairs = sds((tp_count, 2 * tokens, width), bf16)
    flat = sds((tokens, inner), bf16)
    sent = sds((tp_count, tokens, wide), bf16)
    own = sds((tokens, width), bf16)
    share = sds((tokens // 2, 2 * width), bf16)
    stats = sds((tokens, 128), f32)
    gain_own = sds((1, width), f32)
    high = sds((tokens, inner), f32)
    own_share = functools.partial(share_kernel, features)
    dot = 2 * tokens * features * inner

    def prepared(kernel, tick, extra, extra_shape, outs):
        whole = [pl.BlockSpec(v.shape, lambda i, slot, n=len(v.shape): (0,) * n) for v in outs]
        return pl.pallas_call(
            kernel,
            grid_spec=pltpu.PrefetchScalarGridSpec(
                num_scalar_prefetch=1,
                grid=(1,),
                in_specs=[
                    pl.BlockSpec((1, 1, tokens, features), lambda i, slot: (0, slot[0, tick], 0, 0)),
                    pl.BlockSpec((1, features), lambda i, slot: (0, 0)),
                    pl.BlockSpec(extra_shape, lambda i, slot: (0, 0, 0)),
                ],
                out_specs=whole,
            ),
            out_shape=outs,
            cost_estimate=cost(dot, outs, (gain,)),
            compiler_params=pltpu.CompilerParams(vmem_limit_bytes=vmem_budget),
        )(order, stash, gain, extra)

    pair = (tp_count // 2, width, inner)
    w0 = weight[0]
    w2 = swapped(w0, "fsdp", 2)
    one = (1, tokens, features)
    left1, x1, inv1, dy1, gains = prepared(
        prepare_first_kernel, 0, grad_now, one, [pairs, own, stats, own, gain_own]
    )
    h2, x2, inv2, top1 = prepared(
        prepare_second_kernel, 1, grad_top, one, [blocks, own, stats, blocks]
    )
    (w0_late, left1) = lax.optimization_barrier((w0, left1))
    w1 = swapped(w0_late, "fsdp", 1)
    (w2, left1, x1, inv1, dy1, gains, h2, x2, inv2, top1) = lax.optimization_barrier(
        (w2, left1, x1, inv1, dy1, gains, h2, x2, inv2, top1)
    )
    w3 = swapped(w2, "fsdp", 1)
    weights = (w0, w1, w2, w3)

    part1 = call(part_kernel, dot, sds((2 * tokens, inner), f32), left1, w0, w1, w2)
    right1, out1 = call(
        first_kernel, 2 * dot, [sds((2 * tokens, inner), bf16), sent], part1, left1, *weights
    )
    got1 = exchanged(out1)
    share1 = call(own_share, dot // 8, share, got1, x1, inv1, gains, dy1)
    arrived1 = moved_down(share1)
    acc, act2, hidden2, slope2 = call(
        between_kernel,
        3 * dot,
        [sds(pair, f32), flat, high, high],
        left1, right1, h2, *weights,
    )
    (arrived1, acc, act2, hidden2, slope2) = lax.optimization_barrier(
        (arrived1, acc, act2, hidden2, slope2)
    )
    held1 = copied_to_all(arrived1)
    dy2, pre2, out2, dy2_own = call(
        second_kernel,
        2 * dot,
        [blocks, flat, sent, own],
        hidden2, slope2, held1, top1, *weights,
    )
    got2 = exchanged(out2)
    share2 = call(own_share, dot // 8, share, got2, x2, inv2, gains, dy2_own)
    arrived2 = moved_down(share2)
    late_args = (h2, dy2, pre2, act2)
    send = call(late_kernel, dot, sds(pair, bf16), *late_args, acc)
    from_core = swapped(send, "fsdp", 1)
    keep = call(stay_kernel, 2 * dot, sds(pair, f32), left1, right1, *late_args)
    across = keep[1] + from_core[1].astype(f32)
    across = swapped(across.astype(bf16), "fsdp", 2)
    held2 = copied_to_all(arrived2)
    grad_held = call(last_kernel, dot // 8, sds((1, tokens, features), bf16), held2, grad_top)
    weight_grad = keep[0] + from_core[0].astype(f32) + across.astype(f32)
    return (grad_held, weight_grad[None])


def solution(mesh):
    return jax.shard_map(
        per_device,
        mesh=mesh,
        in_specs=(
            P("section", None, "fsdp", None),
            P("section", "fsdp", None),
            P(None, "fsdp", None),
            P("section", None),
            P("section", None),
            P("section", "fsdp", "tp"),
        ),
        out_specs=(P("section", "fsdp", None), P("section", "fsdp", "tp")),
        check_vma=False,
    )
```
